8 devices in a mesh: tp: 8 (over z, y, x, core).
Axes of the slice: x: 2, y: 2, z: 1, core: 2. Of those that a mesh axis runs over, the one named last changes fastest.
Arguments:
- tok_ids: int32 [2, 512], replicated
- next_ids: int32 [2, 512], replicated
- seq_lens: int32 [512], replicated
- embed: bfloat16 [256000, 2048], P('tp')
- ln_gain: bfloat16 [2048], replicated
- w_in: bfloat16 [2048, 35328], P(None, 'tp')
- w_out: bfloat16 [18432, 2048], P('tp')
- final_gain: bfloat16 [2048], replicated
- k_cache: bfloat16 [512, 128, 256], P('tp')
- v_cache: bfloat16 [512, 128, 256], P('tp')
Outputs:
- output 1: float32 [2, 512], replicated
- output 2: bfloat16 [512, 128, 256], P('tp')
- output 3: bfloat16 [512, 128, 256], P('tp')
All inputs are finite; a program needn't handle non-finite values.
Results may differ from the reference program's by a relative error of at most 0.001.
Values are sent between devices in bfloat16 or wider.
A program may use at most 1 GiB of HBM per device.

```python
import jax
import jax.numpy as jnp
from jax import lax

D = 2048
HEADS = 8
HEAD = 256
FF = 16384
VOCAB = 256000
GROUP = 8
BATCH_DEV = 64
CACHE_LEN = 128
NUM_STEPS = 2

BATCH = BATCH_DEV * GROUP
QKV_WIDTH = (HEADS + 2) * HEAD
ATTN_WIDTH = HEADS * HEAD
QKV_DEV = QKV_WIDTH // GROUP
ATTN_DEV = ATTN_WIDTH // GROUP
FF_DEV = FF // GROUP
IN_DEV = QKV_DEV + 2 * FF_DEV
OUT_DEV = ATTN_DEV + FF_DEV
IN_WIDTH = IN_DEV * GROUP
OUT_WIDTH = OUT_DEV * GROUP
MAP_ROWS = min(BATCH, 64)
MAP_COUNT = BATCH // MAP_ROWS
NORM_EPS = 1e-6
ROPE_BASE = 10000.0


def setup_inputs(seed: int = 0) -> dict:
    key_list = jax.random.split(jax.random.key(seed), 11)
    tok_ids = jax.random.randint(key_list[0], (NUM_STEPS, BATCH), 0, VOCAB, dtype=jnp.int32)
    next_ids = jax.random.randint(key_list[1], (NUM_STEPS, BATCH), 0, VOCAB, dtype=jnp.int32)
    base_lens = jax.random.randint(key_list[2], (BATCH,), 0, CACHE_LEN - 1, dtype=jnp.int32)
    perm_order = jax.random.permutation(key_list[3], BATCH)
    seq_lens = base_lens.at[perm_order[0]].set(CACHE_LEN - 2).at[perm_order[1]].set(0)
    embed = jax.random.normal(key_list[4], (VOCAB, D), jnp.float32).astype(jnp.bfloat16)
    ln_gain = (1.0 + 0.3 * jax.random.normal(key_list[5], (D,), jnp.float32)).astype(jnp.bfloat16)
    w_in = (jax.random.normal(key_list[6], (D, IN_WIDTH), jnp.float32) * D ** -0.5).astype(jnp.bfloat16)
    row_scale = jnp.where(jnp.arange(OUT_WIDTH) % OUT_DEV < ATTN_DEV, 2.0 * ATTN_WIDTH ** -0.5, FF ** -0.5)
    w_out = (jax.random.normal(key_list[7], (OUT_WIDTH, D), jnp.float32) * row_scale[:, None]).astype(jnp.bfloat16)
    final_gain = (1.6 * (1.0 + 0.3 * jax.random.normal(key_list[8], (D,), jnp.float32))).astype(jnp.bfloat16)
    k_cache = jax.random.normal(key_list[9], (BATCH, CACHE_LEN, HEAD), jnp.float32).astype(jnp.bfloat16)
    v_cache = jax.random.normal(key_list[10], (BATCH, CACHE_LEN, HEAD), jnp.float32).astype(jnp.bfloat16)
    return {'tok_ids': tok_ids, 'next_ids': next_ids, 'seq_lens': seq_lens, 'embed': embed, 'ln_gain': ln_gain, 'w_in': w_in, 'w_out': w_out, 'final_gain': final_gain, 'k_cache': k_cache, 'v_cache': v_cache}


def layer_norm(values, gain_vec):
    centered = values.astype(jnp.float32)
    centered = centered - jnp.mean(centered, axis=-1, keepdims=True)
    variance = jnp.mean(jnp.square(centered), axis=-1, keepdims=True)
    scaled = centered * lax.rsqrt(variance + NORM_EPS) * gain_vec.astype(jnp.float32)
    return scaled.astype(jnp.bfloat16)


def rotary(vectors, positions):
    half_dim = vectors.shape[-1] // 2
    inv_freq = ROPE_BASE ** (-jnp.arange(half_dim, dtype=jnp.float32) / half_dim)
    angles = positions.astype(jnp.float32)[..., None] * inv_freq
    cosine = jnp.cos(angles)
    sine_val = jnp.sin(angles)
    first_half = vectors[..., :half_dim]
    second_half = vectors[..., half_dim:]
    return jnp.concatenate([first_half * cosine - second_half * sine_val, second_half * cosine + first_half * sine_val], axis=-1)


def block_steps(tok_blk, next_blk, len_blk, k_blk, v_blk, embed, ln_gain, w_in, w_out, final_gain):
    row_count = len_blk.shape[0]
    time_ids = jnp.arange(CACHE_LEN)
    step_logp = []
    for step_idx in range(NUM_STEPS):
        positions = len_blk + step_idx
        x_rows = embed[tok_blk[step_idx]]
        normed = layer_norm(x_rows, ln_gain)
        proj_out = jnp.dot(normed, w_in, preferred_element_type=jnp.float32).astype(jnp.bfloat16)
        proj_out = proj_out.reshape(row_count, GROUP, IN_DEV)
        qkv_vec = proj_out[:, :, :QKV_DEV].reshape(row_count, QKV_WIDTH)
        gate_proj = proj_out[:, :, QKV_DEV:QKV_DEV + FF_DEV].astype(jnp.float32)
        up_proj = proj_out[:, :, QKV_DEV + FF_DEV:].astype(jnp.float32)
        mlp_act = (jax.nn.silu(gate_proj) * up_proj).astype(jnp.bfloat16)
        queries = qkv_vec[:, :ATTN_WIDTH].reshape(row_count, HEADS, HEAD).astype(jnp.float32)
        q_rot = (rotary(queries, positions[:, None]) * HEAD ** -0.5).astype(jnp.bfloat16)
        k_new = rotary(qkv_vec[:, ATTN_WIDTH:ATTN_WIDTH + HEAD].astype(jnp.float32), positions).astype(jnp.bfloat16)
        v_new = qkv_vec[:, ATTN_WIDTH + HEAD:]
        write_mask = time_ids[None, :, None] == positions[:, None, None]
        k_blk = jnp.where(write_mask, k_new[:, None, :], k_blk)
        v_blk = jnp.where(write_mask, v_new[:, None, :], v_blk)
        scores = jnp.einsum('bhd,btd->bht', q_rot.astype(jnp.float32), k_blk.astype(jnp.float32))
        visible = time_ids[None, None, :] <= positions[:, None, None]
        attn_probs = jax.nn.softmax(jnp.where(visible, scores, -jnp.inf), axis=-1).astype(jnp.bfloat16)
        attn_out = jnp.einsum('bht,btd->bhd', attn_probs.astype(jnp.float32), v_blk.astype(jnp.float32)).astype(jnp.bfloat16)
        attn_grp = attn_out.reshape(row_count, GROUP, ATTN_DEV)
        combined = jnp.concatenate([attn_grp, mlp_act], axis=2).reshape(row_count, OUT_WIDTH)
        layer_out = jnp.dot(combined, w_out, preferred_element_type=jnp.float32).astype(jnp.bfloat16)
        resid_sum = x_rows.astype(jnp.float32) + layer_out.astype(jnp.float32)
        final_normed = layer_norm(resid_sum, final_gain)
        logits = jnp.dot(final_normed, embed.T, preferred_element_type=jnp.float32) * D ** -0.5
        picked = jnp.take_along_axis(logits, next_blk[step_idx][:, None], axis=1)[:, 0]
        step_logp.append(picked - jax.nn.logsumexp(logits, axis=1))
    return jnp.stack(step_logp), k_blk, v_blk


def reference(tok_ids, next_ids, seq_lens, embed, ln_gain, w_in, w_out, final_gain, k_cache, v_cache):
    tok_grp = tok_ids.reshape(NUM_STEPS, MAP_COUNT, MAP_ROWS).transpose(1, 0, 2)
    next_grp = next_ids.reshape(NUM_STEPS, MAP_COUNT, MAP_ROWS).transpose(1, 0, 2)
    len_grp = seq_lens.reshape(MAP_COUNT, MAP_ROWS)
    k_grp = k_cache.reshape(MAP_COUNT, MAP_ROWS, CACHE_LEN, HEAD)
    v_grp = v_cache.reshape(MAP_COUNT, MAP_ROWS, CACHE_LEN, HEAD)

    def run_group(group_in):
        return block_steps(group_in[0], group_in[1], group_in[2], group_in[3], group_in[4], embed, ln_gain, w_in, w_out, final_gain)

    logp_grp, k_done, v_done = lax.map(run_group, (tok_grp, next_grp, len_grp, k_grp, v_grp))
    log_probs = logp_grp.transpose(1, 0, 2).reshape(NUM_STEPS, BATCH)
    return log_probs, k_done.reshape(BATCH, CACHE_LEN, HEAD), v_done.reshape(BATCH, CACHE_LEN, HEAD)
```

```python
import functools
import math

import jax
import jax.numpy as jnp
from jax import lax
from jax.experimental import pallas as pl
from jax.experimental.pallas import tpu as pltpu
from jax.sharding import PartitionSpec as P

ROPE_BASE = 10000.0
NORM_EPS = 1e-6
LOG2E = 1.4426950408889634
MESH_ID = pl.DeviceIdType.MESH
F32 = jnp.float32
BF16 = jnp.bfloat16
MIB = 2 ** 20


def norm_rows(values, gain_row):
    centered = values - jnp.mean(values, axis=-1, keepdims=True)
    variance = jnp.mean(jnp.square(centered), axis=-1, keepdims=True)
    return (centered * lax.rsqrt(variance + NORM_EPS) * gain_row.astype(F32)).astype(BF16)


def gather_kernel(count, vocab_dev, ids_ref, embed_ref, out_ref, blocks, rows, wide, slots, sem):
    width = out_ref.shape[1]
    per_loop = 8

    def compact(idx, total):
        for sub in range(per_loop):
            pos = idx * per_loop + sub
            local_id = ids_ref[pos]
            slots[total] = pos
            total = total + jnp.where((local_id >= 0) & (local_id < vocab_dev), 1, 0)
        return total

    total = lax.fori_loop(0, count // per_loop, compact, jnp.int32(0))

    def block_copy(slot):
        local_id = ids_ref[slots[slot]]
        start = pl.multiple_of((local_id // 8) * 8, 8)
        return pltpu.make_async_copy(embed_ref.at[pl.ds(start, 8), :], blocks.at[slot], sem)

    def issue(slot, carry):
        block_copy(slot).start()
        return carry

    lax.fori_loop(0, total, issue, 0)
    rows[...] = jnp.zeros_like(rows)

    def drain(slot, carry):
        pltpu.make_async_copy(embed_ref.at[pl.ds(0, 8), :], blocks.at[slot], sem).wait()
        return carry

    lax.fori_loop(0, total, drain, 0)

    def pick(idx, carry):
        for sub in range(4):
            slot = idx * 4 + sub

            @pl.when(slot < total)
            def _():
                wide[sub] = blocks[slot].astype(F32)

        for sub in range(4):
            slot = idx * 4 + sub

            @pl.when(slot < total)
            def _():
                pos = slots[slot]
                rows[pl.ds(pos, 1), :] = wide[sub, pl.ds(lax.rem(ids_ref[pos], 8), 1), :]

        return carry

    lax.fori_loop(0, (total + 3) // 4, pick, 0)
    out_ref[...] = rows[...].astype(BF16)


def gather_rows(local_ids, embed_loc):
    count = local_ids.shape[0]
    vocab_dev, width = embed_loc.shape
    return pl.pallas_call(
        functools.partial(gather_kernel, count, vocab_dev),
        grid_spec=pltpu.PrefetchScalarGridSpec(
            num_scalar_prefetch=1,
            grid=(1,),
            in_specs=[pl.BlockSpec(memory_space=pl.ANY)],
            out_specs=pl.BlockSpec((count, width), lambda i, ids: (0, 0)),
            scratch_shapes=[
                pltpu.VMEM((count, 8, width), BF16),
                pltpu.VMEM((count, width), F32),
                pltpu.VMEM((4, 8, width), F32),
                pltpu.SMEM((count + 1,), jnp.int32),
                pltpu.SemaphoreType.DMA,
            ],
        ),
        out_shape=jax.ShapeDtypeStruct((count, width), BF16),
        compiler_params=pltpu.CompilerParams(vmem_limit_bytes=60 * MIB),
        name="gather_rows",
    )(local_ids, embed_loc)


def exchange_kernel(chunks, with_base, *refs):
    if with_base:
        part, base, gain, full, pair_buf, send_buf, recv_buf, pair_sems, sum_sems, own_sems, all_sems, fwd_sems = refs
        own = None
    else:
        part, gain, full, own, pair_buf, send_buf, recv_buf, pair_sems, sum_sems, own_sems, all_sems, fwd_sems = refs
    me = lax.axis_index("tp")
    chip, core = me // 2, lax.rem(me, 2)
    other = 1 - core
    mate = chip * 2 + other
    chips = [chip, lax.rem(chip, 2) * (-2) + chip + 1, lax.rem(chip + 2, 4), 3 - chip]
    peers = [chips[k] * 2 + core for k in range(4)]
    size = part.shape[2] // chunks

    barrier = pltpu.get_barrier_semaphore()
    for target in [mate] + peers[1:]:
        pl.semaphore_signal(barrier, inc=1, device_id=(target,), device_id_type=MESH_ID)
    pl.semaphore_wait(barrier, 4)

    def span(c):
        return pl.ds(c * size, size)

    def remote(src, dst, sems, idx, target):
        return pltpu.make_async_remote_copy(
            src_ref=src, dst_ref=dst, send_sem=sems.at[(0,) + idx], recv_sem=sems.at[(1,) + idx],
            device_id=(target,), device_id_type=MESH_ID)

    pair = [remote(part.at[:, other, span(c), :], pair_buf.at[:, span(c), :], pair_sems, (c,), mate) for c in range(chunks)]
    sums = [[remote(send_buf.at[k - 1, span(c), :], recv_buf.at[k - 1, span(c), :], sum_sems, (k - 1, c), peers[k])
             for c in range(chunks)] for k in (1, 2, 3)]
    mine = [full.at[chip, core, span(c), :] for c in range(chunks)]
    give = [remote(mine[c], mine[c], own_sems, (c,), mate) for c in range(chunks)]
    alls = [[remote(mine[c], mine[c], all_sems, (k - 1, c), peers[k]) for c in range(chunks)] for k in (1, 2, 3)]

    def landed(k, c):
        return full.at[chips[k], core, span(c), :]

    fwds = [[remote(landed(k, c), landed(k, c), fwd_sems, (k - 1, c), mate) for c in range(chunks)] for k in (1, 2, 3)]

    for c in range(chunks):
        pair[c].start()
    for c in range(chunks):
        pair[c].wait_recv()
        for k in (3, 1, 2):
            both = part[chips[k], core, span(c), :].astype(F32) + pair_buf[chips[k], span(c), :].astype(F32)
            send_buf[k - 1, span(c), :] = both.astype(BF16)
            sums[k - 1][c].start()
    for c in range(chunks):
        total = part[chip, core, span(c), :].astype(F32) + pair_buf[chip, span(c), :].astype(F32)
        for k in (1, 2, 3):
            sums[k - 1][c].wait_recv()
            total = total + recv_buf[k - 1, span(c), :].astype(F32)
        summed = total.astype(BF16)
        if with_base:
            rows = base[span(c), :].astype(F32) + summed.astype(F32)
        else:
            own[span(c), :] = summed
            rows = summed.astype(F32)
        full[chip, core, span(c), :] = norm_rows(rows, gain[...])
        for k in (3, 1, 2):
            alls[k - 1][c].start()
        give[c].start()
    for c in range(chunks):
        for k in (1, 2, 3):
            alls[k - 1][c].wait_recv()
            fwds[k - 1][c].start()
    for c in range(chunks):
        give[c].wait_recv()
        for k in (1, 2, 3):
            fwds[k - 1][c].wait_recv()
    for c in range(chunks):
        pair[c].wait_send()
        give[c].wait_send()
        for k in (0, 1, 2):
            sums[k][c].wait_send()
            alls[k][c].wait_send()
            fwds[k][c].wait_send()


def exchange(part, base, gain, cid, chunks=4):
    rows, width = part.shape
    own_rows = rows // 8
    vmem = pl.BlockSpec(memory_space=pltpu.VMEM)
    full_shape = jax.ShapeDtypeStruct((4, 2, own_rows, width), BF16)
    with_base = base is not None
    dma = pltpu.SemaphoreType.DMA
    args = [part.reshape(4, 2, own_rows, width)] + ([base] if with_base else []) + [gain.reshape(1, width)]
    out = pl.pallas_call(
        functools.partial(exchange_kernel, chunks, with_base),
        in_specs=[vmem] * len(args),
        out_specs=[vmem] if with_base else [vmem, vmem],
        out_shape=[full_shape] if with_base else [full_shape, jax.ShapeDtypeStruct((own_rows, width), BF16)],
        scratch_shapes=[
            pltpu.VMEM((4, own_rows, width), BF16),
            pltpu.VMEM((3, own_rows, width), BF16),
            pltpu.VMEM((3, own_rows, width), BF16),
            dma((2, chunks)), dma((2, 3, chunks)), dma((2, chunks)), dma((2, 3, chunks)), dma((2, 3, chunks)),
        ],
        compiler_params=pltpu.CompilerParams(collective_id=cid, has_side_effects=True, vmem_limit_bytes=40 * MIB),
        name="exchange_rows",
    )(*args)
    full = out[0].reshape(rows, width)
    return (full, None) if with_base else (full, out[1])


def attention_kernel(seqs, steps, heads, lens_ref, q_ref, kn_ref, vn_ref, k_ref, v_ref, o_ref, ko_ref, vo_ref):
    first = pl.program_id(0) * seqs
    cache_len = k_ref.shape[1]
    head_dim = k_ref.shape[2]
    times = lax.broadcasted_iota(jnp.int32, (cache_len, head_dim), 0)
    qtime = lax.broadcasted_iota(jnp.int32, (steps * heads, cache_len), 1)
    qstep = lax.broadcasted_iota(jnp.int32, (steps * heads, cache_len), 0) // heads
    for b in range(seqs):
        pos = lens_ref[first + b]
        kb = k_ref[b].astype(F32)
        vb = v_ref[b].astype(F32)
        for s in range(steps):
            hit = times == pos + s
            kb = jnp.where(hit, kn_ref[b, s:s + 1, :].astype(F32), kb)
            vb = jnp.where(hit, vn_ref[b, s:s + 1, :].astype(F32), vb)
        kb = kb.astype(BF16)
        vb = vb.astype(BF16)
        ko_ref[b] = kb
        vo_ref[b] = vb
        scores = lax.dot_general(q_ref[b], kb, (((1,), (1,)), ((), ())), preferred_element_type=F32)
        scores = jnp.where(qtime <= pos + qstep, scores, -jnp.inf)
        expd = jnp.exp(scores - jnp.max(scores, axis=-1, keepdims=True))
        probs = (expd / jnp.sum(expd, axis=-1, keepdims=True)).astype(BF16)
        o_ref[b] = jnp.dot(probs, vb, preferred_element_type=F32).astype(BF16)


def attention(own_lens, q_rot, k_new, v_new, k_loc, v_loc, seqs=8):
    batch, cache_len, head_dim = k_loc.shape
    steps = k_new.shape[1]
    queries = q_rot.shape[1]

    def spec(rows):
        return pl.BlockSpec((seqs, rows, head_dim), lambda i, lens: (i, 0, 0))

    return pl.pallas_call(
        functools.partial(attention_kernel, seqs, steps, queries // steps),
        grid_spec=pltpu.PrefetchScalarGridSpec(
            num_scalar_prefetch=1,
            grid=(batch // seqs,),
            in_specs=[spec(queries), spec(steps), spec(steps), spec(cache_len), spec(cache_len)],
            out_specs=[spec(queries), spec(cache_len), spec(cache_len)],
        ),
        out_shape=[
            jax.ShapeDtypeStruct(q_rot.shape, BF16),
            jax.ShapeDtypeStruct(k_loc.shape, BF16),
            jax.ShapeDtypeStruct(v_loc.shape, BF16),
        ],
        compiler_params=pltpu.CompilerParams(vmem_limit_bytes=40 * MIB),
        name="attention_rows",
    )(own_lens, q_rot, k_new, v_new, k_loc, v_loc)


def head_kernel(tile, sub, scale, z_ref, next_ref, e_ref, m_ref, s_ref, t_ref):
    step = pl.program_id(0)
    rows = z_ref.shape[0]

    @pl.when(step == 0)
    def _():
        m_ref[...] = jnp.full_like(m_ref, -jnp.inf)
        s_ref[...] = jnp.zeros_like(s_ref)
        t_ref[...] = jnp.zeros_like(t_ref)

    top, acc, hit = m_ref[...], s_ref[...], t_ref[...]
    wanted = next_ref[...] - step * tile - lax.broadcasted_iota(jnp.int32, (8, rows), 0)
    for part in range(tile // sub):
        dots = lax.dot_general(
            e_ref[part * sub:(part + 1) * sub, :], z_ref[...], (((1,), (1,)), ((), ())), preferred_element_type=F32)
        dots = dots.reshape(sub // 8, 8, rows)
        new_top = jnp.maximum(top, jnp.max(dots, axis=0))
        acc = acc * jnp.exp2((top - new_top) * (scale * LOG2E)) + jnp.sum(
            jnp.exp2((dots - new_top[None]) * (scale * LOG2E)), axis=0)
        top = new_top
        for row in range(sub // 8):
            hit = hit + jnp.where(wanted == part * sub + row * 8, dots[row], 0.0)
    m_ref[...] = top
    s_ref[...] = acc
    t_ref[...] = hit


def head(z_rows, local_next, embed_loc, tile=1280, sub=256):
    rows, width = z_rows.shape
    vocab_dev = embed_loc.shape[0]
    stat = jax.ShapeDtypeStruct((8, rows), F32)
    whole = pl.BlockSpec((8, rows), lambda i: (0, 0))
    return pl.pallas_call(
        functools.partial(head_kernel, tile, sub, width ** -0.5),
        grid=(vocab_dev // tile,),
        in_specs=[
            pl.BlockSpec((rows, width), lambda i: (0, 0)),
            whole,
            pl.BlockSpec((tile, width), lambda i: (i, 0)),
        ],
        out_specs=[whole] * 3,
        out_shape=[stat] * 3,
        compiler_params=pltpu.CompilerParams(vmem_limit_bytes=60 * MIB),
        name="head_rows",
    )(z_rows, jnp.broadcast_to(local_next, (8, rows)), embed_loc)


def solution(mesh):
    group_size = mesh.shape['tp']

    def device_fn(tok_ids, next_ids, seq_lens, embed_loc, ln_gain, w_in_loc, w_out_loc, final_gain, k_loc, v_loc):
        num_steps, batch_size = tok_ids.shape
        batch_dev = batch_size // group_size
        vocab_dev, model_dim = embed_loc.shape
        cache_len, head_dim = k_loc.shape[1:]
        in_dev = w_in_loc.shape[1]
        out_dev = w_out_loc.shape[0]
        kv_dev = 2 * head_dim // group_size
        attn_dev = 2 * out_dev - in_dev + kv_dev
        ff_dev = out_dev - attn_dev
        qkv_dev = attn_dev + kv_dev
        attn_width = attn_dev * group_size
        num_heads = attn_width // head_dim
        own_rows = num_steps * batch_dev
        scale = model_dim ** -0.5
        dev_index = lax.axis_index('tp')
        vocab_start = dev_index * vocab_dev
        own_lens = lax.dynamic_slice_in_dim(seq_lens, dev_index * batch_dev, batch_dev)

        def to_rows(ids):
            return ids.reshape(num_steps, group_size, batch_dev).transpose(1, 0, 2).reshape(-1)

        x_part = gather_rows(to_rows(tok_ids) - vocab_start, embed_loc)
        normed, x_own = exchange(x_part, None, ln_gain, 0)
        proj_out = jnp.dot(normed, w_in_loc, preferred_element_type=F32).astype(BF16)
        gate_proj = proj_out[:, qkv_dev:qkv_dev + ff_dev].astype(F32)
        up_proj = proj_out[:, qkv_dev + ff_dev:].astype(F32)
        mlp_act = (jax.nn.silu(gate_proj) * up_proj).astype(BF16)
        qkv_own = lax.all_to_all(proj_out[:, :qkv_dev], 'tp', 0, 1, tiled=True)
        positions = (own_lens[None, :] + jnp.arange(num_steps)[:, None]).reshape(-1)
        half = head_dim // 2
        inv_freq = ROPE_BASE ** (-jnp.arange(half, dtype=F32) / half)
        angles = positions.astype(F32)[:, None] * inv_freq
        cosine = jnp.cos(angles)[:, None, :]
        sine = jnp.sin(angles)[:, None, :]
        qk = qkv_own[:, :attn_width + head_dim].reshape(own_rows, num_heads + 1, head_dim).astype(F32)
        lo, hi = qk[..., :half], qk[..., half:]
        rot = jnp.concatenate([lo * cosine - hi * sine, hi * cosine + lo * sine], axis=-1)

        def by_seq(rows):
            return rows.reshape(num_steps, batch_dev, -1, head_dim).transpose(1, 0, 2, 3).reshape(batch_dev, -1, head_dim)

        q_rot = by_seq((rot[:, :num_heads] * head_dim ** -0.5).astype(BF16))
        k_new = by_seq(rot[:, num_heads:].astype(BF16))
        v_new = by_seq(qkv_own[:, attn_width + head_dim:])
        attn_out, k_out, v_out = attention(own_lens, q_rot, k_new, v_new, k_loc, v_loc)
        attn_out = attn_out.reshape(batch_dev, num_steps, attn_width).transpose(1, 0, 2).reshape(own_rows, attn_width)
        attn_cols = lax.all_to_all(attn_out, 'tp', 1, 0, tiled=True)
        combined = jnp.concatenate([attn_cols, mlp_act], axis=1)
        part_out = jnp.dot(combined, w_out_loc, preferred_element_type=F32).astype(BF16)
        z_rows, _ = exchange(part_out, x_own, final_gain, 1)
        top, acc, hit = head(z_rows, to_rows(next_ids) - vocab_start, embed_loc)
        row_top = jnp.max(top, axis=0)
        row_acc = jnp.sum(acc * jnp.exp2((top - row_top) * (scale * LOG2E)), axis=0)
        row_hit = jnp.sum(hit, axis=0)
        stats = lax.all_gather(jnp.stack([row_top, row_acc, row_hit]), 'tp')
        all_top = jnp.max(stats[:, 0], axis=0)
        all_acc = jnp.sum(stats[:, 1] * jnp.exp2((stats[:, 0] - all_top) * (scale * LOG2E)), axis=0)
        target = jnp.sum(stats[:, 2], axis=0)
        logp = (target - all_top) * scale - jnp.log(all_acc)
        logp = logp.reshape(group_size, num_steps, batch_dev).transpose(1, 0, 2).reshape(num_steps, batch_size)
        return logp, k_out, v_out

    cache_spec = P('tp', None, None)
    return jax.shard_map(device_fn, mesh=mesh, in_specs=(P(), P(), P(), P('tp', None), P(), P(None, 'tp'), P('tp', None), P(), cache_spec, cache_spec), out_specs=(P(), cache_spec, cache_spec), check_vma=False)
```

```python
import functools
import math

import jax
import jax.numpy as jnp
from jax import lax
from jax.experimental import pallas as pl
from jax.experimental.pallas import tpu as pltpu
from jax.sharding import PartitionSpec as P

ROPE_BASE = 10000.0
NORM_EPS = 1e-6
LOG2E = 1.4426950408889634
MESH_ID = pl.DeviceIdType.MESH
F32 = jnp.float32
BF16 = jnp.bfloat16
MIB = 2 ** 20


def norm_rows(values, gain_row):
    centered = values - jnp.mean(values, axis=-1, keepdims=True)
    variance = jnp.mean(jnp.square(centered), axis=-1, keepdims=True)
    return (centered * lax.rsqrt(variance + NORM_EPS) * gain_row.astype(F32)).astype(BF16)


def gather_kernel(count, vocab_dev, ids_ref, embed_ref, out_ref, blocks, rows, wide, slots, sem):
    width = out_ref.shape[1]
    per_loop = 8

    def compact(idx, total):
        for sub in range(per_loop):
            pos = idx * per_loop + sub
            local_id = ids_ref[pos]
            slots[total] = pos
            total = total + jnp.where((local_id >= 0) & (local_id < vocab_dev), 1, 0)
        return total

    total = lax.fori_loop(0, count // per_loop, compact, jnp.int32(0))

    def block_copy(slot):
        local_id = ids_ref[slots[slot]]
        start = pl.multiple_of((local_id // 8) * 8, 8)
        return pltpu.make_async_copy(embed_ref.at[pl.ds(start, 8), :], blocks.at[slot], sem)

    def issue(slot, carry):
        block_copy(slot).start()
        return carry

    lax.fori_loop(0, total, issue, 0)
    rows[...] = jnp.zeros_like(rows)

    def drain(slot, carry):
        pltpu.make_async_copy(embed_ref.at[pl.ds(0, 8), :], blocks.at[slot], sem).wait()
        return carry

    lax.fori_loop(0, total, drain, 0)

    def pick(idx, carry):
        for sub in range(4):
            slot = idx * 4 + sub

            @pl.when(slot < total)
            def _():
                wide[sub] = blocks[slot].astype(F32)

        for sub in range(4):
            slot = idx * 4 + sub

            @pl.when(slot < total)
            def _():
                pos = slots[slot]
                rows[pl.ds(pos, 1), :] = wide[sub, pl.ds(lax.rem(ids_ref[pos], 8), 1), :]

        return carry

    lax.fori_loop(0, (total + 3) // 4, pick, 0)
    out_ref[...] = rows[...].astype(BF16)


def gather_rows(local_ids, embed_loc):
    count = local_ids.shape[0]
    vocab_dev, width = embed_loc.shape
    return pl.pallas_call(
        functools.partial(gather_kernel, count, vocab_dev),
        grid_spec=pltpu.PrefetchScalarGridSpec(
            num_scalar_prefetch=1,
            grid=(1,),
            in_specs=[pl.BlockSpec(memory_space=pl.ANY)],
            out_specs=pl.BlockSpec((count, width), lambda i, ids: (0, 0)),
            scratch_shapes=[
                pltpu.VMEM((count, 8, width), BF16),
                pltpu.VMEM((count, width), F32),
                pltpu.VMEM((4, 8, width), F32),
                pltpu.SMEM((count + 1,), jnp.int32),
                pltpu.SemaphoreType.DMA,
            ],
        ),
        out_shape=jax.ShapeDtypeStruct((count, width), BF16),
        compiler_params=pltpu.CompilerParams(vmem_limit_bytes=60 * MIB),
        name="gather_rows",
    )(local_ids, embed_loc)


def project_kernel(chunks, qkv_dev, ff_dev, *refs):
    (part, gain, w_ref, own, act, qkv_all, w_buf, full, pair_buf, send_buf, recv_buf, qkv_buf,
     w_sem, pair_sems, sum_sems, own_sems, all_sems, fwd_sems, qkv_sems) = refs
    me = lax.axis_index("tp")
    chip, core = me // 2, lax.rem(me, 2)
    other = 1 - core
    mate = chip * 2 + other
    chips = [chip, lax.rem(chip, 2) * (-2) + chip + 1, lax.rem(chip + 2, 4), 3 - chip]
    peers = [chips[k] * 2 + core for k in range(4)]
    others = [lax.rem(me + k, 8) for k in range(1, 8)]
    width = part.shape[3]
    size = part.shape[2] // chunks
    count = 8 * size

    w_copy = pltpu.make_async_copy(w_ref, w_buf, w_sem)
    w_copy.start()
    barrier = pltpu.get_barrier_semaphore()
    for target in others:
        pl.semaphore_signal(barrier, inc=1, device_id=(target,), device_id_type=MESH_ID)
    pl.semaphore_wait(barrier, 7)

    def span(c):
        return pl.ds(c * size, size)

    def remote(src, dst, sems, idx, target):
        return pltpu.make_async_remote_copy(
            src_ref=src, dst_ref=dst, send_sem=sems.at[(0,) + idx], recv_sem=sems.at[(1,) + idx],
            device_id=(target,), device_id_type=MESH_ID)

    def pair_copy(c):
        return remote(part.at[:, other, span(c), :], pair_buf.at[:, span(c), :], pair_sems, (c,), mate)

    def sum_copy(k, c):
        return remote(send_buf.at[k - 1, span(c), :], recv_buf.at[k - 1, span(c), :], sum_sems, (k - 1, c), peers[k])

    def all_copy(k, c):
        mine = full.at[c, chip, core]
        if k == 0:
            return remote(mine, mine, own_sems, (c,), mate)
        return remote(mine, mine, all_sems, (k - 1, c), peers[k])

    def fwd_copy(k, c):
        there = full.at[c, chips[k], core]
        return remote(there, there, fwd_sems, (k - 1, c), mate)

    def qkv_copy(k, c):
        return remote(qkv_buf.at[c, others[k]], qkv_all.at[me, span(c), :], qkv_sems, (k, c), others[k])

    def send_sums(c):
        pair_copy(c).wait_recv()
        for k in (3, 1, 2):
            both = part[chips[k], core, span(c), :].astype(F32) + pair_buf[chips[k], span(c), :].astype(F32)
            send_buf[k - 1, span(c), :] = both.astype(BF16)
            sum_copy(k, c).start()

    def send_rows(c):
        total = part[chip, core, span(c), :].astype(F32) + pair_buf[chip, span(c), :].astype(F32)
        for k in (1, 2, 3):
            sum_copy(k, c).wait_recv()
            total = total + recv_buf[k - 1, span(c), :].astype(F32)
        summed = total.astype(BF16)
        own[span(c), :] = summed
        full[c, chip, core] = norm_rows(summed.astype(F32), gain[...])
        for k in (3, 1, 2, 0):
            all_copy(k, c).start()

    def forward_rows(c):
        for k in (1, 2, 3):
            all_copy(k, c).wait_recv()
            fwd_copy(k, c).start()

    def project(c):
        all_copy(0, c).wait_recv()
        for k in (1, 2, 3):
            fwd_copy(k, c).wait_recv()
        if c == 0:
            w_copy.wait()
        rows = full[c].reshape(count, width)
        def columns(start, count):
            return lax.dot_general(
                rows, w_buf[pl.ds(start, count), :], (((1,), (1,)), ((), ())), preferred_element_type=F32).astype(BF16)

        qkv_buf[c] = columns(0, qkv_dev).reshape(8, size, qkv_dev)
        qkv_all[me, span(c), :] = qkv_buf[c, me]
        for k in range(7):
            qkv_copy(k, c).start()

        def mlp_tile(t, carry):
            at = pl.multiple_of(t * 256, 256)
            gate = columns(pl.multiple_of(qkv_dev + at, 64), 256).astype(F32)
            up = columns(pl.multiple_of(qkv_dev + ff_dev + at, 64), 256).astype(F32)
            act[:, span(c), pl.ds(at, 256)] = (jax.nn.silu(gate) * up).astype(BF16).reshape(8, size, 256)
            return carry

        lax.fori_loop(0, ff_dev // 256, mlp_tile, 0)

    for c in range(chunks):
        pair_copy(c).start()
    send_sums(0)
    send_sums(1)
    send_rows(0)
    send_sums(2)
    send_rows(1)
    send_sums(3)
    forward_rows(0)
    project(0)
    send_rows(2)
    forward_rows(1)
    project(1)
    send_rows(3)
    forward_rows(2)
    project(2)
    forward_rows(3)
    project(3)
    for c in range(chunks):
        for k in range(7):
            qkv_copy(k, c).wait_recv()
    for c in range(chunks):
        pair_copy(c).wait_send()
        all_copy(0, c).wait_send()
        for k in (1, 2, 3):
            sum_copy(k, c).wait_send()
            all_copy(k, c).wait_send()
            fwd_copy(k, c).wait_send()
        for k in range(7):
            qkv_copy(k, c).wait_send()


def project(part, gain, w_in_loc, qkv_dev, ff_dev, cid, chunks=4):
    rows, width = part.shape
    own_rows = rows // 8
    size = own_rows // chunks
    vmem = pl.BlockSpec(memory_space=pltpu.VMEM)
    dma = pltpu.SemaphoreType.DMA
    return pl.pallas_call(
        functools.partial(project_kernel, chunks, qkv_dev, ff_dev),
        in_specs=[vmem, vmem, pl.BlockSpec(memory_space=pl.ANY)],
        out_specs=[vmem] * 3,
        out_shape=[
            jax.ShapeDtypeStruct((own_rows, width), BF16),
            jax.ShapeDtypeStruct((8, own_rows, ff_dev), BF16),
            jax.ShapeDtypeStruct((8, own_rows, qkv_dev), BF16),
        ],
        scratch_shapes=[
            pltpu.VMEM(w_in_loc.shape[::-1], BF16),
            pltpu.VMEM((chunks, 4, 2, size, width), BF16),
            pltpu.VMEM((4, own_rows, width), BF16),
            pltpu.VMEM((3, own_rows, width), BF16),
            pltpu.VMEM((3, own_rows, width), BF16),
            pltpu.VMEM((chunks, 8, size, qkv_dev), BF16),
            dma, dma((2, chunks)), dma((2, 3, chunks)), dma((2, chunks)), dma((2, 3, chunks)), dma((2, 3, chunks)),
            dma((2, 7, chunks)),
        ],
        compiler_params=pltpu.CompilerParams(collective_id=cid, has_side_effects=True, vmem_limit_bytes=60 * MIB),
        name="project_rows",
    )(part.reshape(4, 2, own_rows, width), gain.reshape(1, width), w_in_loc.T)


def attention_kernel(seqs, steps, heads, lens_ref, q_ref, kn_ref, vn_ref, k_ref, v_ref, o_ref, ko_ref, vo_ref):
    first = pl.program_id(0) * seqs
    cache_len = k_ref.shape[1]
    head_dim = k_ref.shape[2]
    times = lax.broadcasted_iota(jnp.int32, (cache_len, head_dim), 0)
    qtime = lax.broadcasted_iota(jnp.int32, (steps * heads, cache_len), 1)
    qstep = lax.broadcasted_iota(jnp.int32, (steps * heads, cache_len), 0) // heads
    scores = []
    values = []
    for b in range(seqs):
        pos = lens_ref[first + b]
        kb = k_ref[b].astype(F32)
        vb = v_ref[b].astype(F32)
        for s in range(steps):
            hit = times == pos + s
            kb = jnp.where(hit, kn_ref[b, s:s + 1, :].astype(F32), kb)
            vb = jnp.where(hit, vn_ref[b, s:s + 1, :].astype(F32), vb)
        kb = kb.astype(BF16)
        vb = vb.astype(BF16)
        ko_ref[b] = kb
        vo_ref[b] = vb
        dots = lax.dot_general(q_ref[b], kb, (((1,), (1,)), ((), ())), preferred_element_type=F32)
        scores.append(jnp.where(qtime <= pos + qstep, dots, -jnp.inf))
        values.append(vb)
    scores = jnp.concatenate(scores, axis=0)
    expd = jnp.exp(scores - jnp.max(scores, axis=-1, keepdims=True))
    probs = (expd / jnp.sum(expd, axis=-1, keepdims=True)).astype(BF16)
    queries = steps * heads
    for b in range(seqs):
        o_ref[b] = jnp.dot(probs[b * queries:(b + 1) * queries], values[b], preferred_element_type=F32).astype(BF16)


def attention(own_lens, q_rot, k_new, v_new, k_loc, v_loc, seqs=8):
    batch, cache_len, head_dim = k_loc.shape
    steps = k_new.shape[1]
    queries = q_rot.shape[1]

    def spec(rows):
        return pl.BlockSpec((seqs, rows, head_dim), lambda i, lens: (i, 0, 0))

    return pl.pallas_call(
        functools.partial(attention_kernel, seqs, steps, queries // steps),
        grid_spec=pltpu.PrefetchScalarGridSpec(
            num_scalar_prefetch=1,
            grid=(batch // seqs,),
            in_specs=[spec(queries), spec(steps), spec(steps), spec(cache_len), spec(cache_len)],
            out_specs=[spec(queries), spec(cache_len), spec(cache_len)],
        ),
        out_shape=[
            jax.ShapeDtypeStruct(q_rot.shape, BF16),
            jax.ShapeDtypeStruct(k_loc.shape, BF16),
            jax.ShapeDtypeStruct(v_loc.shape, BF16),
        ],
        compiler_params=pltpu.CompilerParams(vmem_limit_bytes=40 * MIB),
        name="attention_rows",
    )(own_lens, q_rot, k_new, v_new, k_loc, v_loc)


def head_kernel(sizes, tiles, subs, when, scale, *refs):
    (part, base, gain, next_a, next_b, e_ref, out_ref, full_a, full_b, pair_buf, send_buf, recv_buf, tops_a, tops_b,
     stat, stat_all, pair_sems, sum_sems, own_sems, all_sems, fwd_sems, stat_sems) = refs
    step = pl.program_id(0)
    me = lax.axis_index("tp")
    chip, core = me // 2, lax.rem(me, 2)
    other = 1 - core
    mate = chip * 2 + other
    chips = [chip, lax.rem(chip, 2) * (-2) + chip + 1, lax.rem(chip + 2, 4), 3 - chip]
    peers = [chips[k] * 2 + core for k in range(4)]
    others = [lax.rem(me + k, 8) for k in range(1, 8)]
    offsets = (0, sizes[0])
    fulls = (full_a, full_b)
    width = part.shape[3]

    def span(g):
        return pl.ds(offsets[g], sizes[g])

    def remote(src, dst, sems, idx, target):
        return pltpu.make_async_remote_copy(
            src_ref=src, dst_ref=dst, send_sem=sems.at[(0,) + idx], recv_sem=sems.at[(1,) + idx],
            device_id=(target,), device_id_type=MESH_ID)

    def pair_copy(g):
        return remote(part.at[:, other, span(g), :], pair_buf.at[:, span(g), :], pair_sems, (g,), mate)

    def sum_copy(k, g):
        return remote(send_buf.at[k - 1, span(g), :], recv_buf.at[k - 1, span(g), :], sum_sems, (k - 1, g), peers[k])

    def all_copy(k, g):
        mine = fulls[g].at[chip, core]
        if k == 0:
            return remote(mine, mine, own_sems, (g,), mate)
        return remote(mine, mine, all_sems, (k - 1, g), peers[k])

    def fwd_copy(k, g):
        there = fulls[g].at[chips[k], core]
        return remote(there, there, fwd_sems, (k - 1, g), mate)

    def stat_copy(k):
        return remote(stat, stat_all.at[me], stat_sems, (k,), others[k])

    def send_sums(g):
        pair_copy(g).wait_recv()
        for k in (3, 1, 2):
            both = part[chips[k], core, span(g), :].astype(F32) + pair_buf[chips[k], span(g), :].astype(F32)
            send_buf[k - 1, span(g), :] = both.astype(BF16)
            sum_copy(k, g).start()

    def send_rows(g):
        total = part[chip, core, span(g), :].astype(F32) + pair_buf[chip, span(g), :].astype(F32)
        for k in (1, 2, 3):
            sum_copy(k, g).wait_recv()
            total = total + recv_buf[k - 1, span(g), :].astype(F32)
        rows = base[span(g), :].astype(F32) + total.astype(BF16).astype(F32)
        fulls[g][chip, core] = norm_rows(rows, gain[...])
        for k in (3, 1, 2, 0):
            all_copy(k, g).start()

    def forward_rows(g):
        for k in (1, 2, 3):
            all_copy(k, g).wait_recv()
            fwd_copy(k, g).start()

    def rows_here(g):
        all_copy(0, g).wait_recv()
        for k in (1, 2, 3):
            fwd_copy(k, g).wait_recv()

    def logits(g, local_step, next_ref, tops):
        count = 8 * sizes[g]
        tile, sub = tiles[g], subs[g]
        z_rows = fulls[g][...].reshape(count, width)

        @pl.when(local_step == 0)
        def _():
            tops[0] = jnp.full_like(tops[0], -jnp.inf)
            tops[1] = jnp.zeros_like(tops[1])
            tops[2] = jnp.zeros_like(tops[2])

        top, acc, hit = tops[0], tops[1], tops[2]
        wanted = next_ref[...] - local_step * tile - lax.broadcasted_iota(jnp.int32, (8, count), 0)
        for idx in range(tile // sub):
            dots = lax.dot_general(
                e_ref[idx * sub:(idx + 1) * sub, :], z_rows, (((1,), (1,)), ((), ())), preferred_element_type=F32)
            dots = dots.reshape(sub // 8, 8, count)
            new_top = jnp.maximum(top, jnp.max(dots, axis=0))
            acc = acc * jnp.exp2((top - new_top) * (scale * LOG2E)) + jnp.sum(
                jnp.exp2((dots - new_top[None]) * (scale * LOG2E)), axis=0)
            top = new_top
            for row in range(sub // 8):
                hit = hit + jnp.where(wanted == idx * sub + row * 8, dots[row], 0.0)
        tops[0] = top
        tops[1] = acc
        tops[2] = hit

    steps_a = when[0]
    last = pl.num_programs(0) - 1

    @pl.when(step == 0)
    def _():
        barrier = pltpu.get_barrier_semaphore()
        for target in others:
            pl.semaphore_signal(barrier, inc=1, device_id=(target,), device_id_type=MESH_ID)
        pl.semaphore_wait(barrier, 7)
        pair_copy(0).start()
        pair_copy(1).start()
        send_sums(0)
        send_rows(0)
        send_sums(1)
        forward_rows(0)
        rows_here(0)

    @pl.when(step == when[1])
    def _():
        send_rows(1)

    @pl.when(step == when[2])
    def _():
        forward_rows(1)

    @pl.when(step < steps_a)
    def _():
        logits(0, step, next_a, tops_a)

    @pl.when(step == steps_a)
    def _():
        rows_here(1)

    @pl.when(step >= steps_a)
    def _():
        logits(1, step - steps_a, next_b, tops_b)

    @pl.when(step == last)
    def _():
        for g, tops in ((0, tops_a), (1, tops_b)):
            cols = slice(8 * offsets[g], 8 * (offsets[g] + sizes[g]))
            top = jnp.max(tops[0], axis=0, keepdims=True)
            stat[0:1, cols] = top
            stat[1:2, cols] = jnp.sum(tops[1] * jnp.exp2((tops[0] - top) * (scale * LOG2E)), axis=0, keepdims=True)
            stat[2:3, cols] = jnp.sum(tops[2], axis=0, keepdims=True)
        for k in range(7):
            stat_copy(k).start()
        stat_all[me] = stat[...]
        for k in range(7):
            stat_copy(k).wait_recv()
        top = stat_all[0, 0:1, :]
        for d in range(1, 8):
            top = jnp.maximum(top, stat_all[d, 0:1, :])
        acc = jnp.zeros_like(top)
        hit = jnp.zeros_like(top)
        for d in range(8):
            acc = acc + stat_all[d, 1:2, :] * jnp.exp2((stat_all[d, 0:1, :] - top) * (scale * LOG2E))
            hit = hit + stat_all[d, 2:3, :]
        out_ref[...] = (hit - top) * scale - jnp.log(acc)
        for k in range(7):
            stat_copy(k).wait_send()
        for g in (0, 1):
            pair_copy(g).wait_send()
            all_copy(0, g).wait_send()
            for k in (1, 2, 3):
                sum_copy(k, g).wait_send()
                all_copy(k, g).wait_send()
                fwd_copy(k, g).wait_send()


def head(part, base, gain, local_next, embed_loc, cid, sizes=(32, 96), tiles=(3200, 3200), subs=(640, 640), when=(10, 4, 8)):
    rows, width = part.shape
    own_rows = rows // 8
    vocab_dev = embed_loc.shape[0]
    steps_a, steps_b = vocab_dev // tiles[0], vocab_dev // tiles[1]
    vmem = pl.BlockSpec(memory_space=pltpu.VMEM)
    per_dev = local_next.reshape(8, own_rows)
    wanted = [jnp.broadcast_to(ids.reshape(1, -1), (8, ids.size)) for ids in (per_dev[:, :sizes[0]], per_dev[:, sizes[0]:])]
    dma = pltpu.SemaphoreType.DMA
    out = pl.pallas_call(
        functools.partial(head_kernel, sizes, tiles, subs, (steps_a,) + when[1:], width ** -0.5),
        grid=(steps_a + steps_b,),
        in_specs=[vmem] * 5 + [pl.BlockSpec((tiles[0], width), lambda i: (lax.rem(i, steps_a), 0))],
        out_specs=vmem,
        out_shape=jax.ShapeDtypeStruct((1, rows), F32),
        scratch_shapes=[
            pltpu.VMEM((4, 2, sizes[0], width), BF16),
            pltpu.VMEM((4, 2, sizes[1], width), BF16),
            pltpu.VMEM((4, own_rows, width), BF16),
            pltpu.VMEM((3, own_rows, width), BF16),
            pltpu.VMEM((3, own_rows, width), BF16),
            pltpu.VMEM((3, 8, 8 * sizes[0]), F32),
            pltpu.VMEM((3, 8, 8 * sizes[1]), F32),
            pltpu.VMEM((8, rows), F32),
            pltpu.VMEM((8, 8, rows), F32),
            dma((2, 2)), dma((2, 3, 2)), dma((2, 2)), dma((2, 3, 2)), dma((2, 3, 2)), dma((2, 7)),
        ],
        compiler_params=pltpu.CompilerParams(collective_id=cid, has_side_effects=True, vmem_limit_bytes=63 * MIB),
        name="head_rows",
    )(part.reshape(4, 2, own_rows, width), base, gain.reshape(1, width), *wanted, embed_loc)
    by_a = out[0, :8 * sizes[0]].reshape(8, sizes[0])
    by_b = out[0, 8 * sizes[0]:].reshape(8, sizes[1])
    return jnp.concatenate([by_a, by_b], axis=1)


def solution(mesh):
    group_size = mesh.shape['tp']

    def device_fn(tok_ids, next_ids, seq_lens, embed_loc, ln_gain, w_in_loc, w_out_loc, final_gain, k_loc, v_loc):
        num_steps, batch_size = tok_ids.shape
        batch_dev = batch_size // group_size
        vocab_dev, model_dim = embed_loc.shape
        cache_len, head_dim = k_loc.shape[1:]
        in_dev = w_in_loc.shape[1]
        out_dev = w_out_loc.shape[0]
        kv_dev = 2 * head_dim // group_size
        attn_dev = 2 * out_dev - in_dev + kv_dev
        ff_dev = out_dev - attn_dev
        qkv_dev = attn_dev + kv_dev
        attn_width = attn_dev * group_size
        num_heads = attn_width // head_dim
        own_rows = num_steps * batch_dev
        dev_index = lax.axis_index('tp')
        vocab_start = dev_index * vocab_dev
        own_lens = lax.dynamic_slice_in_dim(seq_lens, dev_index * batch_dev, batch_dev)

        def to_rows(ids):
            return ids.reshape(num_steps, group_size, batch_dev).transpose(1, 0, 2).reshape(-1)

        x_part = gather_rows(to_rows(tok_ids) - vocab_start, embed_loc)
        x_own, mlp_act, qkv_parts = project(x_part, ln_gain, w_in_loc, qkv_dev, ff_dev, 0)
        qkv_own = qkv_parts.transpose(1, 0, 2).reshape(own_rows, group_size * qkv_dev)
        positions = (own_lens[None, :] + jnp.arange(num_steps)[:, None]).reshape(-1)
        half = head_dim // 2
        inv_freq = ROPE_BASE ** (-jnp.arange(half, dtype=F32) / half)
        angles = positions.astype(F32)[:, None] * inv_freq
        cosine = jnp.cos(angles)[:, None, :]
        sine = jnp.sin(angles)[:, None, :]
        qk = qkv_own[:, :attn_width + head_dim].reshape(own_rows, num_heads + 1, head_dim).astype(F32)
        lo, hi = qk[..., :half], qk[..., half:]
        rot = jnp.concatenate([lo * cosine - hi * sine, hi * cosine + lo * sine], axis=-1)

        def by_seq(rows):
            return rows.reshape(num_steps, batch_dev, -1, head_dim).transpose(1, 0, 2, 3).reshape(batch_dev, -1, head_dim)

        q_rot = by_seq((rot[:, :num_heads] * head_dim ** -0.5).astype(BF16))
        k_new = by_seq(rot[:, num_heads:].astype(BF16))
        v_new = by_seq(qkv_own[:, attn_width + head_dim:])
        attn_out, k_out, v_out = attention(own_lens, q_rot, k_new, v_new, k_loc, v_loc)
        attn_out = attn_out.reshape(batch_dev, num_steps, attn_width).transpose(1, 0, 2).reshape(own_rows, attn_width)
        attn_cols = lax.all_to_all(attn_out, 'tp', 1, 0, tiled=True)
        mlp_act = mlp_act.reshape(group_size * own_rows, ff_dev)
        combined = jnp.concatenate([attn_cols, mlp_act], axis=1)
        part_out = jnp.dot(combined, w_out_loc, preferred_element_type=F32).astype(BF16)
        logp = head(part_out, x_own, final_gain, to_rows(next_ids) - vocab_start, embed_loc, 1)
        logp = logp.reshape(group_size, num_steps, batch_dev).transpose(1, 0, 2).reshape(num_steps, batch_size)
        return logp, k_out, v_out

    cache_spec = P('tp', None, None)
    return jax.shard_map(device_fn, mesh=mesh, in_specs=(P(), P(), P(), P('tp', None), P(), P(None, 'tp'), P('tp', None), P(), cache_spec, cache_spec), out_specs=(P(), cache_spec, cache_spec), check_vma=False)
```

```python
import functools
import math

import jax
import jax.numpy as jnp
from jax import lax
from jax.experimental import pallas as pl
from jax.experimental.pallas import tpu as pltpu
from jax.sharding import PartitionSpec as P

ROPE_BASE = 10000.0
NORM_EPS = 1e-6
LOG2E = 1.4426950408889634
MESH_ID = pl.DeviceIdType.MESH
F32 = jnp.float32
BF16 = jnp.bfloat16
MIB = 2 ** 20


def norm_rows(values, gain_row):
    centered = values - jnp.mean(values, axis=-1, keepdims=True)
    variance = jnp.mean(jnp.square(centered), axis=-1, keepdims=True)
    return (centered * lax.rsqrt(variance + NORM_EPS) * gain_row.astype(F32)).astype(BF16)


def gather_kernel(count, vocab_dev, ids_ref, embed_ref, out_ref, blocks, rows, wide, slots, sem):
    width = out_ref.shape[1]
    per_loop = 16
    group = wide.shape[0]

    def compact(idx, total):
        for sub in range(per_loop):
            pos = idx * per_loop + sub
            local_id = ids_ref[pos]
            slots[total] = pos
            total = total + jnp.where((local_id >= 0) & (local_id < vocab_dev), 1, 0)
        return total

    total = lax.fori_loop(0, count // per_loop, compact, jnp.int32(0))

    def block_copy(slot):
        local_id = ids_ref[slots[slot]]
        start = pl.multiple_of((local_id // 8) * 8, 8)
        return pltpu.make_async_copy(embed_ref.at[pl.ds(start, 8), :], blocks.at[slot], sem)

    def issue(slot, carry):
        block_copy(slot).start()
        return carry

    lax.fori_loop(0, total, issue, 0)
    rows[...] = jnp.zeros_like(rows)

    def drain(slot, carry):
        pltpu.make_async_copy(embed_ref.at[pl.ds(0, 8), :], blocks.at[slot], sem).wait()
        return carry

    lax.fori_loop(0, total, drain, 0)

    def pick(idx, carry):
        found = [slots[jnp.minimum(idx * group + sub, total - 1)] for sub in range(group)]
        for sub in range(group):
            wide[sub] = blocks[jnp.minimum(idx * group + sub, total - 1)].astype(F32)
        for sub in range(group):
            rows[pl.ds(found[sub], 1), :] = wide[sub, pl.ds(lax.rem(ids_ref[found[sub]], 8), 1), :]
        return carry

    lax.fori_loop(0, (total + group - 1) // group, pick, 0)
    out_ref[...] = rows[...].astype(BF16)


def gather_rows(local_ids, embed_loc):
    count = local_ids.shape[0]
    vocab_dev, width = embed_loc.shape
    return pl.pallas_call(
        functools.partial(gather_kernel, count, vocab_dev),
        grid_spec=pltpu.PrefetchScalarGridSpec(
            num_scalar_prefetch=1,
            grid=(1,),
            in_specs=[pl.BlockSpec(memory_space=pl.ANY)],
            out_specs=pl.BlockSpec((count, width), lambda i, ids: (0, 0)),
            scratch_shapes=[
                pltpu.VMEM((count, 8, width), BF16),
                pltpu.VMEM((count, width), F32),
                pltpu.VMEM((8, 8, width), F32),
                pltpu.SMEM((count + 1,), jnp.int32),
                pltpu.SemaphoreType.DMA,
            ],
        ),
        out_shape=jax.ShapeDtypeStruct((count, width), BF16),
        compiler_params=pltpu.CompilerParams(vmem_limit_bytes=60 * MIB),
        name="gather_rows",
    )(local_ids, embed_loc)


def project_kernel(chunks, qkv_dev, ff_dev, *refs):
    (part, gain, w_ref, own, act, qkv_all, w_buf, full, pair_buf, one_send, one_recv, two_send, two_recv, qkv_buf,
     w_sem, pair_sems, one_sems, two_sems, own_sems, near_sems, far_sems, fwd_sems, qkv_sems) = refs
    me = lax.axis_index("tp")
    chip, core = me // 2, lax.rem(me, 2)
    other = 1 - core
    mate = chip * 2 + other
    chips = [chip, lax.rem(chip, 2) * (-2) + chip + 1, lax.rem(chip + 2, 4), 3 - chip]
    peers = [chips[k] * 2 + core for k in range(4)]
    others = [lax.rem(me + k, 8) for k in range(1, 8)]
    width = part.shape[3]
    size = part.shape[2] // chunks
    count = 8 * size

    w_copy = pltpu.make_async_copy(w_ref, w_buf, w_sem)
    w_copy.start()
    barrier = pltpu.get_barrier_semaphore()
    for target in others:
        pl.semaphore_signal(barrier, inc=1, device_id=(target,), device_id_type=MESH_ID)
    pl.semaphore_wait(barrier, 7)

    def span(c):
        return pl.ds(c * size, size)

    def remote(src, dst, sems, idx, target):
        return pltpu.make_async_remote_copy(
            src_ref=src, dst_ref=dst, send_sem=sems.at[(0,) + idx], recv_sem=sems.at[(1,) + idx],
            device_id=(target,), device_id_type=MESH_ID)

    def pair_copy(c):
        return remote(part.at[:, other, span(c), :], pair_buf.at[:, span(c), :], pair_sems, (c,), mate)

    half_cols = width // 2

    def cols(h):
        return slice(h * half_cols, (h + 1) * half_cols)

    def one_copy(h, c):
        return remote(one_send.at[h, :, span(c), :], one_recv.at[h, :, span(c), :], one_sems, (h, c), peers[1 + h])

    def two_copy(h, c):
        return remote(two_send.at[h, span(c), :], two_recv.at[h, span(c), :], two_sems, (h, c), peers[2 - h])

    def give_copy(c):
        mine = full.at[c, chip, core]
        return remote(mine, mine, own_sems, (c,), mate)

    def near_copy(h, c):
        mine = full.at[c, chip, core, :, cols(h)]
        return remote(mine, mine, near_sems, (h, c), peers[2 - h])

    def far_copy(h, j, c):
        block = full.at[c, chips[0 if j == 0 else 2 - h], core, :, cols(h)]
        return remote(block, block, far_sems, (h, j, c), peers[1 + h])

    def fwd_copy(k, c):
        there = full.at[c, chips[k], core]
        return remote(there, there, fwd_sems, (k - 1, c), mate)

    def qkv_copy(k, c):
        return remote(qkv_buf.at[c, others[k]], qkv_all.at[me, span(c), :], qkv_sems, (k, c), others[k])

    def both(k, h, c):
        mine = part[chips[k], core, span(c), cols(h)].astype(F32)
        return mine + pair_buf[chips[k], span(c), cols(h)].astype(F32)

    def sums_one(c):
        pair_copy(c).wait_recv()
        for h in (0, 1):
            one_send[h, 0, span(c), :] = both(1 + h, h, c).astype(BF16)
            one_send[h, 1, span(c), :] = both(3, h, c).astype(BF16)
            one_copy(h, c).start()

    def sums_two(c):
        for h in (0, 1):
            one_copy(h, c).wait_recv()
            two_send[h, span(c), :] = (both(2 - h, h, c) + one_recv[h, 1, span(c), :].astype(F32)).astype(BF16)
            two_copy(h, c).start()

    def send_rows(c):
        totals = []
        for h in (0, 1):
            two_copy(h, c).wait_recv()
            totals.append(both(0, h, c) + one_recv[h, 0, span(c), :].astype(F32) + two_recv[h, span(c), :].astype(F32))
        summed = jnp.concatenate(totals, axis=1).astype(BF16)
        own[span(c), :] = summed
        full[c, chip, core] = norm_rows(summed.astype(F32), gain[...])
        for h in (0, 1):
            near_copy(h, c).start()
            far_copy(h, 0, c).start()
        give_copy(c).start()

    def relay_rows(c):
        for h in (0, 1):
            near_copy(h, c).wait_recv()
            far_copy(h, 1, c).start()

    def forward_rows(c):
        for h in (0, 1):
            for j in (0, 1):
                far_copy(h, j, c).wait_recv()
        for k in (1, 2, 3):
            fwd_copy(k, c).start()

    def project(c):
        give_copy(c).wait_recv()
        for k in (1, 2, 3):
            fwd_copy(k, c).wait_recv()
        if c == 0:
            w_copy.wait()
        rows = full[c].reshape(count, width)
        def columns(start, count):
            return lax.dot_general(
                rows, w_buf[pl.ds(start, count), :], (((1,), (1,)), ((), ())), preferred_element_type=F32).astype(BF16)

        qkv_buf[c] = columns(0, qkv_dev).reshape(8, size, qkv_dev)
        qkv_all[me, span(c), :] = qkv_buf[c, me]
        for k in range(7):
            qkv_copy(k, c).start()

        def mlp_tile(t, carry):
            at = pl.multiple_of(t * 256, 256)
            gate = columns(pl.multiple_of(qkv_dev + at, 64), 256).astype(F32)
            up = columns(pl.multiple_of(qkv_dev + ff_dev + at, 64), 256).astype(F32)
            act[:, span(c), pl.ds(at, 256)] = (jax.nn.silu(gate) * up).astype(BF16).reshape(8, size, 256)
            return carry

        lax.fori_loop(0, ff_dev // 256, mlp_tile, 0)

    for c in range(chunks):
        pair_copy(c).start()
    stages = (sums_one, sums_two, send_rows, relay_rows, forward_rows, project)
    for turn in range(chunks + len(stages) - 1):
        for depth in range(len(stages)):
            if 0 <= turn - depth < chunks:
                stages[depth](turn - depth)
    for c in range(chunks):
        for k in range(7):
            qkv_copy(k, c).wait_recv()
    for c in range(chunks):
        pair_copy(c).wait_send()
        give_copy(c).wait_send()
        for h in (0, 1):
            one_copy(h, c).wait_send()
            two_copy(h, c).wait_send()
            near_copy(h, c).wait_send()
            far_copy(h, 0, c).wait_send()
            far_copy(h, 1, c).wait_send()
        for k in (1, 2, 3):
            fwd_copy(k, c).wait_send()
        for k in range(7):
            qkv_copy(k, c).wait_send()


def project(part, gain, w_in_loc, qkv_dev, ff_dev, cid, chunks=4):
    rows, width = part.shape
    own_rows = rows // 8
    size = own_rows // chunks
    vmem = pl.BlockSpec(memory_space=pltpu.VMEM)
    dma = pltpu.SemaphoreType.DMA
    return pl.pallas_call(
        functools.partial(project_kernel, chunks, qkv_dev, ff_dev),
        in_specs=[vmem, vmem, pl.BlockSpec(memory_space=pl.ANY)],
        out_specs=[vmem] * 3,
        out_shape=[
            jax.ShapeDtypeStruct((own_rows, width), BF16),
            jax.ShapeDtypeStruct((8, own_rows, ff_dev), BF16),
            jax.ShapeDtypeStruct((8, own_rows, qkv_dev), BF16),
        ],
        scratch_shapes=[
            pltpu.VMEM(w_in_loc.shape[::-1], BF16),
            pltpu.VMEM((chunks, 4, 2, size, width), BF16),
            pltpu.VMEM((4, own_rows, width), BF16),
            pltpu.VMEM((2, 2, own_rows, width // 2), BF16),
            pltpu.VMEM((2, 2, own_rows, width // 2), BF16),
            pltpu.VMEM((2, own_rows, width // 2), BF16),
            pltpu.VMEM((2, own_rows, width // 2), BF16),
            pltpu.VMEM((chunks, 8, size, qkv_dev), BF16),
            dma, dma((2, chunks)), dma((2, 2, chunks)), dma((2, 2, chunks)), dma((2, chunks)), dma((2, 2, chunks)),
            dma((2, 2, 2, chunks)), dma((2, 3, chunks)), dma((2, 7, chunks)),
        ],
        compiler_params=pltpu.CompilerParams(collective_id=cid, has_side_effects=True, vmem_limit_bytes=60 * MIB),
        name="project_rows",
    )(part.reshape(4, 2, own_rows, width), gain.reshape(1, width), w_in_loc.T)


def attention_kernel(seqs, steps, heads, lens_ref, q_ref, kn_ref, vn_ref, k_ref, v_ref, o_ref, ko_ref, vo_ref):
    first = pl.program_id(0) * seqs
    cache_len = k_ref.shape[1]
    head_dim = k_ref.shape[2]
    times = lax.broadcasted_iota(jnp.int32, (cache_len, head_dim), 0)
    qtime = lax.broadcasted_iota(jnp.int32, (steps * heads, cache_len), 1)
    qstep = lax.broadcasted_iota(jnp.int32, (steps * heads, cache_len), 0) // heads
    scores = []
    values = []
    for b in range(seqs):
        pos = lens_ref[first + b]
        kb = k_ref[b].astype(F32)
        vb = v_ref[b].astype(F32)
        for s in range(steps):
            hit = times == pos + s
            kb = jnp.where(hit, kn_ref[b, s:s + 1, :].astype(F32), kb)
            vb = jnp.where(hit, vn_ref[b, s:s + 1, :].astype(F32), vb)
        kb = kb.astype(BF16)
        vb = vb.astype(BF16)
        ko_ref[b] = kb
        vo_ref[b] = vb
        dots = lax.dot_general(q_ref[b], kb, (((1,), (1,)), ((), ())), preferred_element_type=F32)
        scores.append(jnp.where(qtime <= pos + qstep, dots, -jnp.inf))
        values.append(vb)
    scores = jnp.concatenate(scores, axis=0)
    expd = jnp.exp(scores - jnp.max(scores, axis=-1, keepdims=True))
    probs = (expd / jnp.sum(expd, axis=-1, keepdims=True)).astype(BF16)
    queries = steps * heads
    for b in range(seqs):
        o_ref[b] = jnp.dot(probs[b * queries:(b + 1) * queries], values[b], preferred_element_type=F32).astype(BF16)


def attention(own_lens, q_rot, k_new, v_new, k_loc, v_loc, seqs=16):
    batch, cache_len, head_dim = k_loc.shape
    steps = k_new.shape[1]
    queries = q_rot.shape[1]

    def spec(rows):
        return pl.BlockSpec((seqs, rows, head_dim), lambda i, lens: (i, 0, 0))

    return pl.pallas_call(
        functools.partial(attention_kernel, seqs, steps, queries // steps),
        grid_spec=pltpu.PrefetchScalarGridSpec(
            num_scalar_prefetch=1,
            grid=(batch // seqs,),
            in_specs=[spec(queries), spec(steps), spec(steps), spec(cache_len), spec(cache_len)],
            out_specs=[spec(queries), spec(cache_len), spec(cache_len)],
        ),
        out_shape=[
            jax.ShapeDtypeStruct(q_rot.shape, BF16),
            jax.ShapeDtypeStruct(k_loc.shape, BF16),
            jax.ShapeDtypeStruct(v_loc.shape, BF16),
        ],
        compiler_params=pltpu.CompilerParams(vmem_limit_bytes=63 * MIB),
        name="attention_rows",
    )(own_lens, q_rot, k_new, v_new, k_loc, v_loc)


def head_kernel(sizes, tiles, subs, when, scale, *refs):
    (attn, act, base, gain, next_ref, w_ref, e_ref, out_ref, w_buf, attn_all, part, full_a, full_b, pair_buf, send_buf, recv_buf, tops_a, tops_b,
     stat, stat_all, w_sem, attn_sems, pair_sems, sum_sems, own_sems, all_sems, fwd_sems, stat_sems) = refs
    step = pl.program_id(0)
    me = lax.axis_index("tp")
    chip, core = me // 2, lax.rem(me, 2)
    other = 1 - core
    mate = chip * 2 + other
    chips = [chip, lax.rem(chip, 2) * (-2) + chip + 1, lax.rem(chip + 2, 4), 3 - chip]
    peers = [chips[k] * 2 + core for k in range(4)]
    others = [lax.rem(me + k, 8) for k in range(1, 8)]
    offsets = (0, sizes[0])
    fulls = (full_a, full_b)
    width = base.shape[1]

    def span(g):
        return pl.ds(offsets[g], sizes[g])

    def remote(src, dst, sems, idx, target):
        return pltpu.make_async_remote_copy(
            src_ref=src, dst_ref=dst, send_sem=sems.at[(0,) + idx], recv_sem=sems.at[(1,) + idx],
            device_id=(target,), device_id_type=MESH_ID)

    def pair_copy(g):
        return remote(part.at[:, other, span(g), :], pair_buf.at[:, span(g), :], pair_sems, (g,), mate)

    def sum_copy(k, g):
        return remote(send_buf.at[k - 1, span(g), :], recv_buf.at[k - 1, span(g), :], sum_sems, (k - 1, g), peers[k])

    def all_copy(k, g):
        mine = fulls[g].at[chip, core]
        if k == 0:
            return remote(mine, mine, own_sems, (g,), mate)
        return remote(mine, mine, all_sems, (k - 1, g), peers[k])

    def fwd_copy(k, g):
        there = fulls[g].at[chips[k], core]
        return remote(there, there, fwd_sems, (k - 1, g), mate)

    def attn_copy(k, g):
        return remote(attn.at[others[k], span(g), :], attn_all.at[me, span(g), :], attn_sems, (k, g), others[k])

    def project_out(g):
        count = 8 * sizes[g]
        mixed = attn_all.shape[2]
        if g == 0:
            attn_all[me] = attn[me]
        for k in range(7):
            attn_copy(k, g).wait_recv()

        def tile(t, carry):
            cols = pl.ds(pl.multiple_of(t * 512, 512), 512)
            out = jnp.dot(act[:, span(g), :].reshape(count, act.shape[2]), w_buf[mixed:, cols], preferred_element_type=F32)
            out = out + jnp.dot(attn_all[:, span(g), :].reshape(count, mixed), w_buf[:mixed, cols], preferred_element_type=F32)
            part[:, :, span(g), cols] = out.astype(BF16).reshape(4, 2, sizes[g], 512)
            return carry

        lax.fori_loop(0, width // 512, tile, 0)

    def stat_copy(k):
        return remote(stat, stat_all.at[me], stat_sems, (k,), others[k])

    def send_sums(g):
        pair_copy(g).wait_recv()
        for k in (3, 1, 2):
            both = part[chips[k], core, span(g), :].astype(F32) + pair_buf[chips[k], span(g), :].astype(F32)
            send_buf[k - 1, span(g), :] = both.astype(BF16)
            sum_copy(k, g).start()

    def send_rows(g):
        total = part[chip, core, span(g), :].astype(F32) + pair_buf[chip, span(g), :].astype(F32)
        for k in (1, 2, 3):
            sum_copy(k, g).wait_recv()
            total = total + recv_buf[k - 1, span(g), :].astype(F32)
        rows = base[span(g), :].astype(F32) + total.astype(BF16).astype(F32)
        fulls[g][chip, core] = norm_rows(rows, gain[...])
        for k in (3, 1, 2, 0):
            all_copy(k, g).start()

    def forward_rows(g):
        for k in (1, 2, 3):
            all_copy(k, g).wait_recv()
            fwd_copy(k, g).start()

    def rows_here(g):
        all_copy(0, g).wait_recv()
        for k in (1, 2, 3):
            fwd_copy(k, g).wait_recv()

    def logits(g, local_step, tops):
        count = 8 * sizes[g]
        tile, sub = tiles[g], subs[g]
        z_rows = fulls[g][...].reshape(count, width)

        @pl.when(local_step == 0)
        def _():
            tops[0] = jnp.full_like(tops[0], -jnp.inf)
            tops[1] = jnp.zeros_like(tops[1])
            tops[2] = jnp.zeros_like(tops[2])

        top, acc, hit = tops[0], tops[1], tops[2]
        wanted = next_ref[:, 8 * offsets[g]:8 * offsets[g] + count] - local_step * tile - lax.broadcasted_iota(jnp.int32, (8, count), 0)
        for idx in range(tile // sub):
            dots = lax.dot_general(
                e_ref[idx * sub:(idx + 1) * sub, :], z_rows, (((1,), (1,)), ((), ())), preferred_element_type=F32)
            dots = dots.reshape(sub // 8, 8, count)
            new_top = jnp.maximum(top, jnp.max(dots, axis=0))
            acc = acc * jnp.exp2((top - new_top) * (scale * LOG2E)) + jnp.sum(
                jnp.exp2((dots - new_top[None]) * (scale * LOG2E)), axis=0)
            top = new_top
            for row in range(sub // 8):
                hit = hit + jnp.where(wanted == idx * sub + row * 8, dots[row], 0.0)
        tops[0] = top
        tops[1] = acc
        tops[2] = hit

    steps_a = when[0]
    last = pl.num_programs(0) - 1

    @pl.when(step == 0)
    def _():
        w_copy = pltpu.make_async_copy(w_ref, w_buf, w_sem)
        w_copy.start()
        barrier = pltpu.get_barrier_semaphore()
        for target in others:
            pl.semaphore_signal(barrier, inc=1, device_id=(target,), device_id_type=MESH_ID)
        pl.semaphore_wait(barrier, 7)
        for g in (0, 1):
            for k in range(7):
                attn_copy(k, g).start()
        w_copy.wait()
        project_out(0)
        pair_copy(0).start()
        send_sums(0)
        project_out(1)
        pair_copy(1).start()
        send_rows(0)
        send_sums(1)
        forward_rows(0)
        rows_here(0)

    @pl.when(step == when[1])
    def _():
        send_rows(1)

    @pl.when(step == when[2])
    def _():
        forward_rows(1)

    @pl.when(step < steps_a)
    def _():
        logits(0, step, tops_a)

    @pl.when(step == steps_a)
    def _():
        rows_here(1)

    @pl.when(step >= steps_a)
    def _():
        logits(1, step - steps_a, tops_b)

    @pl.when(step == last)
    def _():
        for g, tops in ((0, tops_a), (1, tops_b)):
            cols = slice(8 * offsets[g], 8 * (offsets[g] + sizes[g]))
            top = jnp.max(tops[0], axis=0, keepdims=True)
            stat[0:1, cols] = top
            stat[1:2, cols] = jnp.sum(tops[1] * jnp.exp2((tops[0] - top) * (scale * LOG2E)), axis=0, keepdims=True)
            stat[2:3, cols] = jnp.sum(tops[2], axis=0, keepdims=True)
        for k in range(7):
            stat_copy(k).start()
        stat_all[me] = stat[...]
        for k in range(7):
            stat_copy(k).wait_recv()
        top = stat_all[0, 0:1, :]
        for d in range(1, 8):
            top = jnp.maximum(top, stat_all[d, 0:1, :])
        acc = jnp.zeros_like(top)
        hit = jnp.zeros_like(top)
        for d in range(8):
            acc = acc + stat_all[d, 1:2, :] * jnp.exp2((stat_all[d, 0:1, :] - top) * (scale * LOG2E))
            hit = hit + stat_all[d, 2:3, :]
        out_ref[...] = (hit - top) * scale - jnp.log(acc)
        for k in range(7):
            stat_copy(k).wait_send()
        for g in (0, 1):
            for k in range(7):
                attn_copy(k, g).wait_send()
            pair_copy(g).wait_send()
            all_copy(0, g).wait_send()
            for k in (1, 2, 3):
                sum_copy(k, g).wait_send()
                all_copy(k, g).wait_send()
                fwd_copy(k, g).wait_send()


def head(attn, act, base, gain, local_next, w_out_loc, embed_loc, cid, sizes=(32, 96), tiles=(3200, 3200), subs=(640, 640), when=(10, 4, 8)):
    own_rows, width = base.shape
    rows = own_rows * 8
    vocab_dev = embed_loc.shape[0]
    steps_a, steps_b = vocab_dev // tiles[0], vocab_dev // tiles[1]
    vmem = pl.BlockSpec(memory_space=pltpu.VMEM)
    per_dev = local_next.reshape(8, own_rows)
    wanted = jnp.concatenate([per_dev[:, :sizes[0]].reshape(-1), per_dev[:, sizes[0]:].reshape(-1)])
    wanted = jnp.broadcast_to(wanted, (8, rows))
    dma = pltpu.SemaphoreType.DMA
    out = pl.pallas_call(
        functools.partial(head_kernel, sizes, tiles, subs, (steps_a,) + when[1:], width ** -0.5),
        grid=(steps_a + steps_b,),
        in_specs=[vmem] * 5 + [pl.BlockSpec(memory_space=pl.ANY), pl.BlockSpec((tiles[0], width), lambda i: (lax.rem(i, steps_a), 0))],
        out_specs=vmem,
        out_shape=jax.ShapeDtypeStruct((1, rows), F32),
        scratch_shapes=[
            pltpu.VMEM(w_out_loc.shape, BF16),
            pltpu.VMEM(attn.shape, BF16),
            pltpu.VMEM((4, 2, own_rows, width), BF16),
            pltpu.VMEM((4, 2, sizes[0], width), BF16),
            pltpu.VMEM((4, 2, sizes[1], width), BF16),
            pltpu.VMEM((4, own_rows, width), BF16),
            pltpu.VMEM((3, own_rows, width), BF16),
            pltpu.VMEM((3, own_rows, width), BF16),
            pltpu.VMEM((3, 8, 8 * sizes[0]), F32),
            pltpu.VMEM((3, 8, 8 * sizes[1]), F32),
            pltpu.VMEM((8, rows), F32),
            pltpu.VMEM((8, 8, rows), F32),
            dma, dma((2, 7, 2)), dma((2, 2)), dma((2, 3, 2)), dma((2, 2)), dma((2, 3, 2)), dma((2, 3, 2)), dma((2, 7)),
        ],
        compiler_params=pltpu.CompilerParams(collective_id=cid, has_side_effects=True, vmem_limit_bytes=63 * MIB),
        name="head_rows",
    )(attn, act, base, gain.reshape(1, width), wanted, w_out_loc, embed_loc)
    by_a = out[0, :8 * sizes[0]].reshape(8, sizes[0])
    by_b = out[0, 8 * sizes[0]:].reshape(8, sizes[1])
    return jnp.concatenate([by_a, by_b], axis=1)


def solution(mesh):
    group_size = mesh.shape['tp']

    def device_fn(tok_ids, next_ids, seq_lens, embed_loc, ln_gain, w_in_loc, w_out_loc, final_gain, k_loc, v_loc):
        num_steps, batch_size = tok_ids.shape
        batch_dev = batch_size // group_size
        vocab_dev, model_dim = embed_loc.shape
        cache_len, head_dim = k_loc.shape[1:]
        in_dev = w_in_loc.shape[1]
        out_dev = w_out_loc.shape[0]
        kv_dev = 2 * head_dim // group_size
        attn_dev = 2 * out_dev - in_dev + kv_dev
        ff_dev = out_dev - attn_dev
        qkv_dev = attn_dev + kv_dev
        attn_width = attn_dev * group_size
        num_heads = attn_width // head_dim
        own_rows = num_steps * batch_dev
        dev_index = lax.axis_index('tp')
        vocab_start = dev_index * vocab_dev
        own_lens = lax.dynamic_slice_in_dim(seq_lens, dev_index * batch_dev, batch_dev)

        def to_rows(ids):
            return ids.reshape(num_steps, group_size, batch_dev).transpose(1, 0, 2).reshape(-1)

        x_part = gather_rows(to_rows(tok_ids) - vocab_start, embed_loc)
        x_own, mlp_act, qkv_parts = project(x_part, ln_gain, w_in_loc, qkv_dev, ff_dev, 0)
        qkv_own = qkv_parts.transpose(1, 0, 2).reshape(own_rows, group_size * qkv_dev)
        positions = (own_lens[None, :] + jnp.arange(num_steps)[:, None]).reshape(-1)
        half = head_dim // 2
        inv_freq = ROPE_BASE ** (-jnp.arange(half, dtype=F32) / half)
        angles = positions.astype(F32)[:, None] * inv_freq
        cosine = jnp.cos(angles)[:, None, :]
        sine = jnp.sin(angles)[:, None, :]
        qk = qkv_own[:, :attn_width + head_dim].reshape(own_rows, num_heads + 1, head_dim).astype(F32)
        lo, hi = qk[..., :half], qk[..., half:]
        rot = jnp.concatenate([lo * cosine - hi * sine, hi * cosine + lo * sine], axis=-1)

        def by_seq(rows):
            return rows.reshape(num_steps, batch_dev, -1, head_dim).transpose(1, 0, 2, 3).reshape(batch_dev, -1, head_dim)

        q_rot = by_seq((rot[:, :num_heads] * head_dim ** -0.5).astype(BF16))
        k_new = by_seq(rot[:, num_heads:].astype(BF16))
        v_new = by_seq(qkv_own[:, attn_width + head_dim:])
        attn_out, k_out, v_out = attention(own_lens, q_rot, k_new, v_new, k_loc, v_loc)
        attn_parts = attn_out.reshape(batch_dev, num_steps, group_size, attn_dev).transpose(2, 1, 0, 3)
        attn_parts = attn_parts.reshape(group_size, own_rows, attn_dev)
        local_next = to_rows(next_ids) - vocab_start
        logp = head(attn_parts, mlp_act, x_own, final_gain, local_next, w_out_loc, embed_loc, 1)
        logp = logp.reshape(group_size, num_steps, batch_dev).transpose(1, 0, 2).reshape(num_steps, batch_size)
        return logp, k_out, v_out

    cache_spec = P('tp', None, None)
    return jax.shard_map(device_fn, mesh=mesh, in_specs=(P(), P(), P(), P('tp', None), P(), P(None, 'tp'), P('tp', None), P(), cache_spec, cache_spec), out_specs=(P(), cache_spec, cache_spec), check_vma=False)
```

```python
import functools
import math

import jax
import jax.numpy as jnp
from jax import lax
from jax.experimental import pallas as pl
from jax.experimental.pallas import tpu as pltpu
from jax.sharding import PartitionSpec as P

ROPE_BASE = 10000.0
NORM_EPS = 1e-6
LOG2E = 1.4426950408889634
MESH_ID = pl.DeviceIdType.MESH
F32 = jnp.float32
BF16 = jnp.bfloat16
MIB = 2 ** 20


def norm_rows(values, gain_row):
    centered = values - jnp.mean(values, axis=-1, keepdims=True)
    variance = jnp.mean(jnp.square(centered), axis=-1, keepdims=True)
    return (centered * lax.rsqrt(variance + NORM_EPS) * gain_row.astype(F32)).astype(BF16)


def gather_kernel(count, vocab_dev, ids_ref, embed_ref, out_ref, blocks, rows, wide, slots, sem):
    width = out_ref.shape[1]
    per_loop = 16
    group = wide.shape[0]

    def compact(idx, total):
        for sub in range(per_loop):
            pos = idx * per_loop + sub
            local_id = ids_ref[pos]
            slots[total] = pos
            total = total + jnp.where((local_id >= 0) & (local_id < vocab_dev), 1, 0)
        return total

    total = lax.fori_loop(0, count // per_loop, compact, jnp.int32(0))

    def block_copy(slot):
        local_id = ids_ref[slots[slot]]
        start = pl.multiple_of((local_id // 8) * 8, 8)
        return pltpu.make_async_copy(embed_ref.at[pl.ds(start, 8), :], blocks.at[slot], sem)

    def issue(slot, carry):
        block_copy(slot).start()
        return carry

    lax.fori_loop(0, total, issue, 0)
    rows[...] = jnp.zeros_like(rows)

    def drain(slot, carry):
        pltpu.make_async_copy(embed_ref.at[pl.ds(0, 8), :], blocks.at[slot], sem).wait()
        return carry

    lax.fori_loop(0, total, drain, 0)

    def pick(idx, carry):
        found = [slots[jnp.minimum(idx * group + sub, total - 1)] for sub in range(group)]
        for sub in range(group):
            wide[sub] = blocks[jnp.minimum(idx * group + sub, total - 1)].astype(F32)
        for sub in range(group):
            rows[pl.ds(found[sub], 1), :] = wide[sub, pl.ds(lax.rem(ids_ref[found[sub]], 8), 1), :]
        return carry

    lax.fori_loop(0, (total + group - 1) // group, pick, 0)
    out_ref[...] = rows[...].astype(BF16)


def gather_rows(local_ids, embed_loc):
    count = local_ids.shape[0]
    vocab_dev, width = embed_loc.shape
    return pl.pallas_call(
        functools.partial(gather_kernel, count, vocab_dev),
        grid_spec=pltpu.PrefetchScalarGridSpec(
            num_scalar_prefetch=1,
            grid=(1,),
            in_specs=[pl.BlockSpec(memory_space=pl.ANY)],
            out_specs=pl.BlockSpec((count, width), lambda i, ids: (0, 0)),
            scratch_shapes=[
                pltpu.VMEM((count, 8, width), BF16),
                pltpu.VMEM((count, width), F32),
                pltpu.VMEM((8, 8, width), F32),
                pltpu.SMEM((count + 1,), jnp.int32),
                pltpu.SemaphoreType.DMA,
            ],
        ),
        out_shape=jax.ShapeDtypeStruct((count, width), BF16),
        compiler_params=pltpu.CompilerParams(vmem_limit_bytes=60 * MIB),
        name="gather_rows",
    )(local_ids, embed_loc)


def project_kernel(chunks, qkv_dev, ff_dev, *refs):
    (part, gain, w_ref, own, act, qkv_all, w_buf, full, pair_buf, one_send, one_recv, two_send, two_recv, qkv_buf,
     w_sem, pair_sems, one_sems, two_sems, own_sems, near_sems, far_sems, fwd_sems, qkv_sems) = refs
    me = lax.axis_index("tp")
    chip, core = me // 2, lax.rem(me, 2)
    other = 1 - core
    mate = chip * 2 + other
    chips = [chip, lax.rem(chip, 2) * (-2) + chip + 1, lax.rem(chip + 2, 4), 3 - chip]
    peers = [chips[k] * 2 + core for k in range(4)]
    others = [lax.rem(me + k, 8) for k in range(1, 8)]
    width = part.shape[3]
    size = part.shape[2] // chunks
    count = 8 * size

    w_copy = pltpu.make_async_copy(w_ref, w_buf, w_sem)
    w_copy.start()
    barrier = pltpu.get_barrier_semaphore()
    for target in others:
        pl.semaphore_signal(barrier, inc=1, device_id=(target,), device_id_type=MESH_ID)
    pl.semaphore_wait(barrier, 7)

    def span(c):
        return pl.ds(c * size, size)

    def remote(src, dst, sems, idx, target):
        return pltpu.make_async_remote_copy(
            src_ref=src, dst_ref=dst, send_sem=sems.at[(0,) + idx], recv_sem=sems.at[(1,) + idx],
            device_id=(target,), device_id_type=MESH_ID)

    def pair_copy(c):
        return remote(part.at[:, other, span(c), :], pair_buf.at[:, span(c), :], pair_sems, (c,), mate)

    half_cols = width // 2

    def cols(h):
        return slice(h * half_cols, (h + 1) * half_cols)

    def one_copy(h, c):
        return remote(one_send.at[h, :, span(c), :], one_recv.at[h, :, span(c), :], one_sems, (h, c), peers[1 + h])

    def two_copy(h, c):
        return remote(two_send.at[h, span(c), :], two_recv.at[h, span(c), :], two_sems, (h, c), peers[2 - h])

    def give_copy(c):
        mine = full.at[c, chip, core]
        return remote(mine, mine, own_sems, (c,), mate)

    def near_copy(h, c):
        mine = full.at[c, chip, core, :, cols(h)]
        return remote(mine, mine, near_sems, (h, c), peers[2 - h])

    def far_copy(h, j, c):
        block = full.at[c, chips[0 if j == 0 else 2 - h], core, :, cols(h)]
        return remote(block, block, far_sems, (h, j, c), peers[1 + h])

    def fwd_copy(k, c):
        there = full.at[c, chips[k], core]
        return remote(there, there, fwd_sems, (k - 1, c), mate)

    def qkv_copy(k, c):
        return remote(qkv_buf.at[c, others[k]], qkv_all.at[me, span(c), :], qkv_sems, (k, c), others[k])

    def both(k, h, c):
        mine = part[chips[k], core, span(c), cols(h)].astype(F32)
        return mine + pair_buf[chips[k], span(c), cols(h)].astype(F32)

    def sums_one(c):
        pair_copy(c).wait_recv()
        for h in (0, 1):
            one_send[h, 0, span(c), :] = both(1 + h, h, c).astype(BF16)
            one_send[h, 1, span(c), :] = both(3, h, c).astype(BF16)
            one_copy(h, c).start()

    def sums_two(c):
        for h in (0, 1):
            one_copy(h, c).wait_recv()
            two_send[h, span(c), :] = (both(2 - h, h, c) + one_recv[h, 1, span(c), :].astype(F32)).astype(BF16)
            two_copy(h, c).start()

    def send_rows(c):
        totals = []
        for h in (0, 1):
            two_copy(h, c).wait_recv()
            totals.append(both(0, h, c) + one_recv[h, 0, span(c), :].astype(F32) + two_recv[h, span(c), :].astype(F32))
        summed = jnp.concatenate(totals, axis=1).astype(BF16)
        own[span(c), :] = summed
        full[c, chip, core] = norm_rows(summed.astype(F32), gain[...])
        for h in (0, 1):
            near_copy(h, c).start()
            far_copy(h, 0, c).start()
        give_copy(c).start()

    def relay_rows(c):
        for h in (0, 1):
            near_copy(h, c).wait_recv()
            far_copy(h, 1, c).start()

    def forward_rows(c):
        for h in (0, 1):
            for j in (0, 1):
                far_copy(h, j, c).wait_recv()
        for k in (1, 2, 3):
            fwd_copy(k, c).start()

    def project(c):
        give_copy(c).wait_recv()
        for k in (1, 2, 3):
            fwd_copy(k, c).wait_recv()
        if c == 0:
            w_copy.wait()
        rows = full[c].reshape(count, width)
        def columns(start, count):
            return lax.dot_general(
                rows, w_buf[pl.ds(start, count), :], (((1,), (1,)), ((), ())), preferred_element_type=F32).astype(BF16)

        qkv_buf[c] = columns(0, qkv_dev).reshape(8, size, qkv_dev)
        qkv_all[me, span(c), :] = qkv_buf[c, me]
        for k in range(7):
            qkv_copy(k, c).start()

        def mlp_tile(t, carry):
            at = pl.multiple_of(t * 256, 256)
            gate = columns(pl.multiple_of(qkv_dev + at, 64), 256).astype(F32)
            up = columns(pl.multiple_of(qkv_dev + ff_dev + at, 64), 256).astype(F32)
            act[:, span(c), pl.ds(at, 256)] = (jax.nn.silu(gate) * up).astype(BF16).reshape(8, size, 256)
            return carry

        lax.fori_loop(0, ff_dev // 256, mlp_tile, 0)

    for c in range(chunks):
        pair_copy(c).start()
    stages = (sums_one, sums_two, send_rows, relay_rows, forward_rows, project)
    for turn in range(chunks + len(stages) - 1):
        for depth in range(len(stages)):
            if 0 <= turn - depth < chunks:
                stages[depth](turn - depth)
    for c in range(chunks):
        for k in range(7):
            qkv_copy(k, c).wait_recv()
    for c in range(chunks):
        pair_copy(c).wait_send()
        give_copy(c).wait_send()
        for h in (0, 1):
            one_copy(h, c).wait_send()
            two_copy(h, c).wait_send()
            near_copy(h, c).wait_send()
            far_copy(h, 0, c).wait_send()
            far_copy(h, 1, c).wait_send()
        for k in (1, 2, 3):
            fwd_copy(k, c).wait_send()
        for k in range(7):
            qkv_copy(k, c).wait_send()


def project(part, gain, w_in_loc, qkv_dev, ff_dev, cid, chunks=4):
    rows, width = part.shape
    own_rows = rows // 8
    size = own_rows // chunks
    vmem = pl.BlockSpec(memory_space=pltpu.VMEM)
    dma = pltpu.SemaphoreType.DMA
    return pl.pallas_call(
        functools.partial(project_kernel, chunks, qkv_dev, ff_dev),
        in_specs=[vmem, vmem, pl.BlockSpec(memory_space=pl.ANY)],
        out_specs=[vmem] * 3,
        out_shape=[
            jax.ShapeDtypeStruct((own_rows, width), BF16),
            jax.ShapeDtypeStruct((8, own_rows, ff_dev), BF16),
            jax.ShapeDtypeStruct((8, own_rows, qkv_dev), BF16),
        ],
        scratch_shapes=[
            pltpu.VMEM(w_in_loc.shape[::-1], BF16),
            pltpu.VMEM((chunks, 4, 2, size, width), BF16),
            pltpu.VMEM((4, own_rows, width), BF16),
            pltpu.VMEM((2, 2, own_rows, width // 2), BF16),
            pltpu.VMEM((2, 2, own_rows, width // 2), BF16),
            pltpu.VMEM((2, own_rows, width // 2), BF16),
            pltpu.VMEM((2, own_rows, width // 2), BF16),
            pltpu.VMEM((chunks, 8, size, qkv_dev), BF16),
            dma, dma((2, chunks)), dma((2, 2, chunks)), dma((2, 2, chunks)), dma((2, chunks)), dma((2, 2, chunks)),
            dma((2, 2, 2, chunks)), dma((2, 3, chunks)), dma((2, 7, chunks)),
        ],
        compiler_params=pltpu.CompilerParams(collective_id=cid, has_side_effects=True, vmem_limit_bytes=60 * MIB),
        name="project_rows",
    )(part.reshape(4, 2, own_rows, width), gain.reshape(1, width), w_in_loc.T)


def attention_kernel(seqs, steps, heads, lens_ref, q_ref, kn_ref, vn_ref, k_ref, v_ref, o_ref, ko_ref, vo_ref):
    first = pl.program_id(0) * seqs
    cache_len = k_ref.shape[1]
    head_dim = k_ref.shape[2]
    times = lax.broadcasted_iota(jnp.int32, (cache_len, head_dim), 0)
    qtime = lax.broadcasted_iota(jnp.int32, (steps * heads, cache_len), 1)
    qstep = lax.broadcasted_iota(jnp.int32, (steps * heads, cache_len), 0) // heads
    scores = []
    values = []
    for b in range(seqs):
        pos = lens_ref[first + b]
        kb = k_ref[b].astype(F32)
        vb = v_ref[b].astype(F32)
        for s in range(steps):
            hit = times == pos + s
            kb = jnp.where(hit, kn_ref[b, s:s + 1, :].astype(F32), kb)
            vb = jnp.where(hit, vn_ref[b, s:s + 1, :].astype(F32), vb)
        kb = kb.astype(BF16)
        vb = vb.astype(BF16)
        ko_ref[b] = kb
        vo_ref[b] = vb
        dots = lax.dot_general(q_ref[b], kb, (((1,), (1,)), ((), ())), preferred_element_type=F32)
        scores.append(jnp.where(qtime <= pos + qstep, dots, -jnp.inf))
        values.append(vb)
    scores = jnp.concatenate(scores, axis=0)
    expd = jnp.exp(scores - jnp.max(scores, axis=-1, keepdims=True))
    probs = (expd / jnp.sum(expd, axis=-1, keepdims=True)).astype(BF16)
    queries = steps * heads
    for b in range(seqs):
        o_ref[b] = jnp.dot(probs[b * queries:(b + 1) * queries], values[b], preferred_element_type=F32).astype(BF16)


def attention(own_lens, q_rot, k_new, v_new, k_loc, v_loc, seqs=16):
    batch, cache_len, head_dim = k_loc.shape
    steps = k_new.shape[1]
    queries = q_rot.shape[1]

    def spec(rows):
        return pl.BlockSpec((seqs, rows, head_dim), lambda i, lens: (i, 0, 0))

    return pl.pallas_call(
        functools.partial(attention_kernel, seqs, steps, queries // steps),
        grid_spec=pltpu.PrefetchScalarGridSpec(
            num_scalar_prefetch=1,
            grid=(batch // seqs,),
            in_specs=[spec(queries), spec(steps), spec(steps), spec(cache_len), spec(cache_len)],
            out_specs=[spec(queries), spec(cache_len), spec(cache_len)],
        ),
        out_shape=[
            jax.ShapeDtypeStruct(q_rot.shape, BF16),
            jax.ShapeDtypeStruct(k_loc.shape, BF16),
            jax.ShapeDtypeStruct(v_loc.shape, BF16),
        ],
        compiler_params=pltpu.CompilerParams(vmem_limit_bytes=63 * MIB),
        name="attention_rows",
    )(own_lens, q_rot, k_new, v_new, k_loc, v_loc)


def head_kernel(sizes, tile, subs, tile_count, when, scale, *refs):
    (attn, base, gain, next_ref, act_ref, w_ref, e_ref, out_ref, e_buf, act, w_buf, attn_all, part, full_a, full_b, pair_buf, send_buf, recv_buf, tops_a, tops_b,
     stat, stat_all, e_sems, act_sem, w_sem, attn_sems, pair_sems, sum_sems, own_sems, all_sems, fwd_sems, stat_sems) = refs
    step = pl.program_id(0)
    me = lax.axis_index("tp")
    chip, core = me // 2, lax.rem(me, 2)
    other = 1 - core
    mate = chip * 2 + other
    chips = [chip, lax.rem(chip, 2) * (-2) + chip + 1, lax.rem(chip + 2, 4), 3 - chip]
    peers = [chips[k] * 2 + core for k in range(4)]
    others = [lax.rem(me + k, 8) for k in range(1, 8)]
    offsets = (0, sizes[0])
    fulls = (full_a, full_b)
    width = base.shape[1]

    def span(g):
        return pl.ds(offsets[g], sizes[g])

    def remote(src, dst, sems, idx, target):
        return pltpu.make_async_remote_copy(
            src_ref=src, dst_ref=dst, send_sem=sems.at[(0,) + idx], recv_sem=sems.at[(1,) + idx],
            device_id=(target,), device_id_type=MESH_ID)

    def pair_copy(g):
        return remote(part.at[:, other, span(g), :], pair_buf.at[:, span(g), :], pair_sems, (g,), mate)

    def sum_copy(k, g):
        return remote(send_buf.at[k - 1, span(g), :], recv_buf.at[k - 1, span(g), :], sum_sems, (k - 1, g), peers[k])

    def all_copy(k, g):
        mine = fulls[g].at[chip, core]
        if k == 0:
            return remote(mine, mine, own_sems, (g,), mate)
        return remote(mine, mine, all_sems, (k - 1, g), peers[k])

    def fwd_copy(k, g):
        there = fulls[g].at[chips[k], core]
        return remote(there, there, fwd_sems, (k - 1, g), mate)

    def attn_copy(k, g):
        return remote(attn.at[others[k], span(g), :], attn_all.at[me, span(g), :], attn_sems, (k, g), others[k])

    def project_out(g):
        count = 8 * sizes[g]
        mixed = attn_all.shape[2]
        if g == 0:
            attn_all[me] = attn[me]
        for k in range(7):
            attn_copy(k, g).wait_recv()

        def tile(t, carry):
            cols = pl.ds(pl.multiple_of(t * 512, 512), 512)
            out = jnp.dot(act[:, span(g), :].reshape(count, act.shape[2]), w_buf[mixed:, cols], preferred_element_type=F32)
            out = out + jnp.dot(attn_all[:, span(g), :].reshape(count, mixed), w_buf[:mixed, cols], preferred_element_type=F32)
            part[:, :, span(g), cols] = out.astype(BF16).reshape(4, 2, sizes[g], 512)
            return carry

        lax.fori_loop(0, width // 512, tile, 0)

    def stat_copy(k):
        return remote(stat, stat_all.at[me], stat_sems, (k,), others[k])

    def send_sums(g):
        pair_copy(g).wait_recv()
        for k in (3, 1, 2):
            both = part[chips[k], core, span(g), :].astype(F32) + pair_buf[chips[k], span(g), :].astype(F32)
            send_buf[k - 1, span(g), :] = both.astype(BF16)
            sum_copy(k, g).start()

    def send_rows(g):
        total = part[chip, core, span(g), :].astype(F32) + pair_buf[chip, span(g), :].astype(F32)
        for k in (1, 2, 3):
            sum_copy(k, g).wait_recv()
            total = total + recv_buf[k - 1, span(g), :].astype(F32)
        rows = base[span(g), :].astype(F32) + total.astype(BF16).astype(F32)
        fulls[g][chip, core] = norm_rows(rows, gain[...])
        for k in (3, 1, 2, 0):
            all_copy(k, g).start()

    def forward_rows(g):
        for k in (1, 2, 3):
            all_copy(k, g).wait_recv()
            fwd_copy(k, g).start()

    def rows_here(g):
        all_copy(0, g).wait_recv()
        for k in (1, 2, 3):
            fwd_copy(k, g).wait_recv()

    def tile_copy(at):
        start = pl.multiple_of(lax.rem(at, tile_count) * tile, tile)
        return pltpu.make_async_copy(e_ref.at[pl.ds(start, tile), :], e_buf.at[lax.rem(at, 2)], e_sems.at[lax.rem(at, 2)])

    def logits(g, first, tops):
        count = 8 * sizes[g]
        sub = subs[g]
        slot = lax.rem(step, 2)
        z_rows = fulls[g][...].reshape(count, width)

        @pl.when(step == first)
        def _():
            tops[0] = jnp.full_like(tops[0], -jnp.inf)
            tops[1] = jnp.zeros_like(tops[1])
            tops[2] = jnp.zeros_like(tops[2])

        top, acc, hit = tops[0], tops[1], tops[2]
        wanted = next_ref[:, 8 * offsets[g]:8 * offsets[g] + count] - lax.rem(step, tile_count) * tile - lax.broadcasted_iota(jnp.int32, (8, count), 0)
        for idx in range(tile // sub):
            dots = lax.dot_general(
                e_buf[slot, idx * sub:(idx + 1) * sub, :], z_rows, (((1,), (1,)), ((), ())), preferred_element_type=F32)
            dots = dots.reshape(sub // 8, 8, count)
            new_top = jnp.maximum(top, jnp.max(dots, axis=0))
            acc = acc * jnp.exp2((top - new_top) * (scale * LOG2E)) + jnp.sum(
                jnp.exp2((dots - new_top[None]) * (scale * LOG2E)), axis=0)
            top = new_top
            for row in range(sub // 8):
                hit = jnp.where(wanted == idx * sub + row * 8, dots[row], hit)
        tops[0] = top
        tops[1] = acc
        tops[2] = hit

    last = pl.num_programs(0) - 1

    @pl.when(step == 0)
    def _():
        w_copy = pltpu.make_async_copy(w_ref, w_buf, w_sem)
        w_copy.start()
        act_copy = pltpu.make_async_copy(act_ref, act, act_sem)
        act_copy.start()
        tile_copy(0).start()
        tile_copy(1).start()
        barrier = pltpu.get_barrier_semaphore()
        for target in others:
            pl.semaphore_signal(barrier, inc=1, device_id=(target,), device_id_type=MESH_ID)
        pl.semaphore_wait(barrier, 7)
        for g in (0, 1):
            for k in range(7):
                attn_copy(k, g).start()
        w_copy.wait()
        act_copy.wait()
        project_out(0)
        pair_copy(0).start()
        send_sums(0)
        project_out(1)
        pair_copy(1).start()
        send_rows(0)
        send_sums(1)
        forward_rows(0)
        rows_here(0)

    @pl.when(step == when[0])
    def _():
        send_rows(1)

    @pl.when(step == when[1])
    def _():
        forward_rows(1)

    @pl.when(step == when[2])
    def _():
        rows_here(1)

    tile_copy(step).wait()

    @pl.when(step < tile_count)
    def _():
        logits(0, 0, tops_a)

    @pl.when(step >= when[2])
    def _():
        logits(1, when[2], tops_b)

    @pl.when(step + 2 <= last)
    def _():
        tile_copy(step + 2).start()

    @pl.when(step == last)
    def _():
        for g, tops in ((0, tops_a), (1, tops_b)):
            cols = slice(8 * offsets[g], 8 * (offsets[g] + sizes[g]))
            top = jnp.max(tops[0], axis=0, keepdims=True)
            stat[0:1, cols] = top
            stat[1:2, cols] = jnp.sum(tops[1] * jnp.exp2((tops[0] - top) * (scale * LOG2E)), axis=0, keepdims=True)
            stat[2:3, cols] = jnp.sum(tops[2], axis=0, keepdims=True)
        for k in range(7):
            stat_copy(k).start()
        stat_all[me] = stat[...]
        for k in range(7):
            stat_copy(k).wait_recv()
        top = stat_all[0, 0:1, :]
        for d in range(1, 8):
            top = jnp.maximum(top, stat_all[d, 0:1, :])
        acc = jnp.zeros_like(top)
        hit = jnp.zeros_like(top)
        for d in range(8):
            acc = acc + stat_all[d, 1:2, :] * jnp.exp2((stat_all[d, 0:1, :] - top) * (scale * LOG2E))
            hit = hit + stat_all[d, 2:3, :]
        out_ref[...] = (hit - top) * scale - jnp.log(acc)
        for k in range(7):
            stat_copy(k).wait_send()
        for g in (0, 1):
            for k in range(7):
                attn_copy(k, g).wait_send()
            pair_copy(g).wait_send()
            all_copy(0, g).wait_send()
            for k in (1, 2, 3):
                sum_copy(k, g).wait_send()
                all_copy(k, g).wait_send()
                fwd_copy(k, g).wait_send()


def head(attn, act, base, gain, local_next, w_out_loc, embed_loc, cid, sizes=(32, 96), tile=3200, subs=(640, 640), when=(4, 7, 8)):
    own_rows, width = base.shape
    rows = own_rows * 8
    vocab_dev = embed_loc.shape[0]
    tile_count = vocab_dev // tile
    vmem = pl.BlockSpec(memory_space=pltpu.VMEM)
    per_dev = local_next.reshape(8, own_rows)
    wanted = jnp.concatenate([per_dev[:, :sizes[0]].reshape(-1), per_dev[:, sizes[0]:].reshape(-1)])
    wanted = jnp.broadcast_to(wanted, (8, rows))
    dma = pltpu.SemaphoreType.DMA
    out = pl.pallas_call(
        functools.partial(head_kernel, sizes, tile, subs, tile_count, when, width ** -0.5),
        grid=(tile_count + when[2],),
        in_specs=[vmem] * 4 + [pl.BlockSpec(memory_space=pl.ANY)] * 3,
        out_specs=vmem,
        out_shape=jax.ShapeDtypeStruct((1, rows), F32),
        scratch_shapes=[
            pltpu.VMEM((2, tile, width), BF16),
            pltpu.VMEM(act.shape, BF16),
            pltpu.VMEM(w_out_loc.shape, BF16),
            pltpu.VMEM(attn.shape, BF16),
            pltpu.VMEM((4, 2, own_rows, width), BF16),
            pltpu.VMEM((4, 2, sizes[0], width), BF16),
            pltpu.VMEM((4, 2, sizes[1], width), BF16),
            pltpu.VMEM((4, own_rows, width), BF16),
            pltpu.VMEM((3, own_rows, width), BF16),
            pltpu.VMEM((3, own_rows, width), BF16),
            pltpu.VMEM((3, 8, 8 * sizes[0]), F32),
            pltpu.VMEM((3, 8, 8 * sizes[1]), F32),
            pltpu.VMEM((8, rows), F32),
            pltpu.VMEM((8, 8, rows), F32),
            dma((2,)), dma, dma, dma((2, 7, 2)), dma((2, 2)), dma((2, 3, 2)), dma((2, 2)), dma((2, 3, 2)), dma((2, 3, 2)), dma((2, 7)),
        ],
        compiler_params=pltpu.CompilerParams(collective_id=cid, has_side_effects=True, vmem_limit_bytes=63 * MIB),
        name="head_rows",
    )(attn, base, gain.reshape(1, width), wanted, act, w_out_loc, embed_loc)
    by_a = out[0, :8 * sizes[0]].reshape(8, sizes[0])
    by_b = out[0, 8 * sizes[0]:].reshape(8, sizes[1])
    return jnp.concatenate([by_a, by_b], axis=1)


def solution(mesh):
    group_size = mesh.shape['tp']

    def device_fn(tok_ids, next_ids, seq_lens, embed_loc, ln_gain, w_in_loc, w_out_loc, final_gain, k_loc, v_loc):
        num_steps, batch_size = tok_ids.shape
        batch_dev = batch_size // group_size
        vocab_dev, model_dim = embed_loc.shape
        cache_len, head_dim = k_loc.shape[1:]
        in_dev = w_in_loc.shape[1]
        out_dev = w_out_loc.shape[0]
        kv_dev = 2 * head_dim // group_size
        attn_dev = 2 * out_dev - in_dev + kv_dev
        ff_dev = out_dev - attn_dev
        qkv_dev = attn_dev + kv_dev
        attn_width = attn_dev * group_size
        num_heads = attn_width // head_dim
        own_rows = num_steps * batch_dev
        dev_index = lax.axis_index('tp')
        vocab_start = dev_index * vocab_dev
        own_lens = lax.dynamic_slice_in_dim(seq_lens, dev_index * batch_dev, batch_dev)

        def to_rows(ids):
            return ids.reshape(num_steps, group_size, batch_dev).transpose(1, 0, 2).reshape(-1)

        x_part = gather_rows(to_rows(tok_ids) - vocab_start, embed_loc)
        x_own, mlp_act, qkv_parts = project(x_part, ln_gain, w_in_loc, qkv_dev, ff_dev, 0)
        qkv_own = qkv_parts.transpose(1, 0, 2).reshape(own_rows, group_size * qkv_dev)
        positions = (own_lens[None, :] + jnp.arange(num_steps)[:, None]).reshape(-1)
        half = head_dim // 2
        inv_freq = ROPE_BASE ** (-jnp.arange(half, dtype=F32) / half)
        angles = positions.astype(F32)[:, None] * inv_freq
        cosine = jnp.cos(angles)[:, None, :]
        sine = jnp.sin(angles)[:, None, :]
        qk = qkv_own[:, :attn_width + head_dim].reshape(own_rows, num_heads + 1, head_dim).astype(F32)
        lo, hi = qk[..., :half], qk[..., half:]
        rot = jnp.concatenate([lo * cosine - hi * sine, hi * cosine + lo * sine], axis=-1)

        def by_seq(rows):
            return rows.reshape(num_steps, batch_dev, -1, head_dim).transpose(1, 0, 2, 3).reshape(batch_dev, -1, head_dim)

        q_rot = by_seq((rot[:, :num_heads] * head_dim ** -0.5).astype(BF16))
        k_new = by_seq(rot[:, num_heads:].astype(BF16))
        v_new = by_seq(qkv_own[:, attn_width + head_dim:])
        attn_out, k_out, v_out = attention(own_lens, q_rot, k_new, v_new, k_loc, v_loc)
        attn_parts = attn_out.reshape(batch_dev, num_steps, group_size, attn_dev).transpose(2, 1, 0, 3)
        attn_parts = attn_parts.reshape(group_size, own_rows, attn_dev)
        local_next = to_rows(next_ids) - vocab_start
        logp = head(attn_parts, mlp_act, x_own, final_gain, local_next, w_out_loc, embed_loc, 1)
        logp = logp.reshape(group_size, num_steps, batch_dev).transpose(1, 0, 2).reshape(num_steps, batch_size)
        return logp, k_out, v_out

    cache_spec = P('tp', None, None)
    return jax.shard_map(device_fn, mesh=mesh, in_specs=(P(), P(), P(), P('tp', None), P(), P(None, 'tp'), P('tp', None), P(), cache_spec, cache_spec), out_specs=(P(), cache_spec, cache_spec), check_vma=False)
```
